8 devices in a mesh: dp: 1 (over z), tp: 8 (over x, y, core).
Axes of the slice: x: 2, y: 2, z: 1, core: 2. Of those that a mesh axis runs over, the one named last changes fastest.
Arguments:
- x: bfloat16 [64, 2048], P('dp')
- k_cache: bfloat16 [64, 4096, 16, 128], P('dp', None, 'tp')
- v_cache: bfloat16 [64, 4096, 16, 128], P('dp', None, 'tp')
- gain_a: bfloat16 [2048], replicated
- wq: bfloat16 [2048, 2048], P(None, 'tp')
- wo: bfloat16 [2048, 2048], P('tp')
- gain_m: bfloat16 [2048], replicated
- w_gate: bfloat16 [2048, 8192], P(None, 'tp')
- w_up: bfloat16 [2048, 8192], P(None, 'tp')
- w_down: bfloat16 [8192, 2048], P('tp')
Outputs:
- output: bfloat16 [64, 2048], P('dp')
All inputs are finite; a program needn't handle non-finite values.
Results may differ from the reference program's by a relative error of at most 0.017.
Values are sent between devices in bfloat16 or wider.
A program may use at most 2 GiB of HBM per device.

```python
import jax
import jax.numpy as jnp
from jax import lax

BATCH = 64
CACHE = 4096
D = 2048
HEADS = 16
KV_HEADS = 16
HEAD = 128
FF = 8192
THETA = 10000


def setup_inputs(seed: int = 0, part: int = 0) -> dict:
    kx, kc, kw, kn, kq, ko, km, kg, ku, kd = jax.random.split(jax.random.key(seed), 10)
    kx, kc, kw = (jax.random.fold_in(k, part) for k in (kx, kc, kw))

    def weights(key, rows, columns):
        return jax.random.normal(key, (rows, columns), jnp.float32) * rows**-0.5

    drawn = {
        "x": jax.random.normal(kx, (BATCH, D), jnp.float32),
        "k_cache": 2 * jax.random.normal(kc, (BATCH, CACHE, KV_HEADS, HEAD), jnp.float32),
        "v_cache": 4 * jax.random.normal(kw, (BATCH, CACHE, KV_HEADS, HEAD), jnp.float32),
        "gain_a": 1 + 0.1 * jax.random.normal(kn, (D,), jnp.float32),
        "wq": 2 * weights(kq, D, HEADS * HEAD),
        "wo": weights(ko, HEADS * HEAD, D),
        "gain_m": 1 + 0.1 * jax.random.normal(km, (D,), jnp.float32),
        "w_gate": weights(kg, D, FF),
        "w_up": weights(ku, D, FF),
        "w_down": 2 * weights(kd, FF, D),
    }
    return {k: v.astype(jnp.bfloat16) for k, v in drawn.items()}


def normed(x, gain):
    wide = x.astype(jnp.float32)
    scale = lax.rsqrt(jnp.mean(wide * wide, -1, keepdims=True) + 1e-6)
    return (wide * scale * gain.astype(jnp.float32)).astype(jnp.bfloat16)


def turned(t, place, theta):
    half = t.shape[-1] // 2
    angle = place.astype(jnp.float32)[:, None] * theta ** (-jnp.arange(half, dtype=jnp.float32) / half)
    cos, sin = jnp.cos(angle)[:, None], jnp.sin(angle)[:, None]
    a, b = t[..., :half].astype(jnp.float32), t[..., half:].astype(jnp.float32)
    return jnp.concatenate([a * cos - b * sin, b * cos + a * sin], -1).astype(jnp.bfloat16)


def matmul(a, w):
    return jnp.dot(a, w, preferred_element_type=jnp.float32).astype(jnp.bfloat16)


def einsum(form, a, b):
    return jnp.einsum(form, a.astype(jnp.float32), b.astype(jnp.float32))


def seen_by(a, wq, k_cache, v_cache, head, theta):
    batch, cache, kv_heads = k_cache.shape[:3]
    place = jnp.full((batch,), cache - 1)
    q = turned(matmul(a, wq).reshape(batch, -1, head), place, theta).reshape(batch, kv_heads, -1, head)
    scores = einsum("bgsd,bugd->bgsu", q, k_cache) * head**-0.5
    weights = jax.nn.softmax(scores, -1).astype(jnp.bfloat16)
    return einsum("bgsu,bugd->bgsd", weights, v_cache).astype(jnp.bfloat16).reshape(batch, -1)


def hidden_of(b, w_gate, w_up):
    gate = jnp.dot(b, w_gate, preferred_element_type=jnp.float32)
    up = jnp.dot(b, w_up, preferred_element_type=jnp.float32)
    return (jax.nn.silu(gate) * up).astype(jnp.bfloat16)


def reference(x, k_cache, v_cache, gain_a, wq, wo, gain_m, w_gate, w_up, w_down):
    seen = seen_by(normed(x, gain_a), wq, k_cache, v_cache, HEAD, THETA)
    h = (x.astype(jnp.float32) + jnp.dot(seen, wo, preferred_element_type=jnp.float32)).astype(jnp.bfloat16)
    hidden = hidden_of(normed(h, gain_m), w_gate, w_up)
    return (h.astype(jnp.float32) + jnp.dot(hidden, w_down, preferred_element_type=jnp.float32)).astype(jnp.bfloat16)
```

```python
import functools

import jax
import jax.numpy as jnp
from jax import lax
from jax.experimental import pallas as pl
from jax.experimental.pallas import tpu as pltpu
from jax.sharding import PartitionSpec as P

HEAD = 128
THETA = 10000
F32, BF16 = jnp.float32, jnp.bfloat16
LOG2E = 1.4426950408889634
NK = NV = 6


def normed(x, gain):
    wide = x.astype(jnp.float32)
    scale = lax.rsqrt(jnp.mean(wide * wide, -1, keepdims=True) + 1e-6)
    return (wide * scale * gain.astype(jnp.float32)).astype(jnp.bfloat16)


def turned(t, place, theta):
    half = t.shape[-1] // 2
    angle = place.astype(jnp.float32)[:, None] * theta ** (-jnp.arange(half, dtype=jnp.float32) / half)
    cos, sin = jnp.cos(angle)[:, None], jnp.sin(angle)[:, None]
    a, b = t[..., :half].astype(jnp.float32), t[..., half:].astype(jnp.float32)
    return jnp.concatenate([a * cos - b * sin, b * cos + a * sin], -1).astype(jnp.bfloat16)


def matmul(a, w):
    return jnp.dot(a, w, preferred_element_type=jnp.float32).astype(jnp.bfloat16)


def hidden_of(b, w_gate, w_up):
    gate = jnp.dot(b, w_gate, preferred_element_type=jnp.float32)
    up = jnp.dot(b, w_up, preferred_element_type=jnp.float32)
    return (jax.nn.silu(gate) * up).astype(jnp.bfloat16)


def scores_of(q_ref, kbuf, s_ref, b, slot, par, tiles):
    row = q_ref[pl.ds(b, 1), :]
    q0 = jnp.broadcast_to(row[:, :HEAD], (16, HEAD))
    q1 = jnp.broadcast_to(row[:, HEAD:], (16, HEAD))
    r = lax.broadcasted_iota(jnp.int32, (16, HEAD), 0)
    q = jnp.where((r & 1) == 0, q0, q1)
    first = (r & 2) == 0
    lhs = jnp.concatenate([jnp.where(first, q, 0.0), jnp.where(first, 0.0, q)], 1).astype(BF16)
    for j in range(tiles):
        ka = kbuf[slot, 512 * j : 512 * j + 256, :]
        kb = kbuf[slot, 512 * j + 256 : 512 * j + 512, :]
        s = lax.dot_general(lhs, jnp.concatenate([ka, kb], 1), (((1,), (1,)), ((), ())), preferred_element_type=F32)
        s_ref[par, :, 256 * j : 256 * j + 256] = s[:8]


def seen_from(s_ref, vbuf, seen_ref, b, slot, par, tiles):
    r = lax.broadcasted_iota(jnp.int32, (8, 256), 0)
    c = lax.broadcasted_iota(jnp.int32, (8, 256), 1)
    mine = (r & 1) == (c & 1)
    t = [jnp.where(mine, s_ref[par, :, 256 * j : 256 * j + 256], -1e30) for j in range(tiles)]
    m = functools.reduce(jnp.maximum, t)
    m = jnp.max(jnp.maximum(m[:, :128], m[:, 128:]), 1, keepdims=True)
    m = jnp.broadcast_to(m, (8, 128))
    m = jnp.maximum(m, pltpu.roll(m, 2, 0))
    m = jnp.concatenate([m, m], 1)
    k = HEAD**-0.5 * LOG2E
    p = [jnp.exp2((x - m) * k) for x in t]
    l = functools.reduce(jnp.add, p)
    l = jnp.sum(l[:, :128] + l[:, 128:], 1, keepdims=True)
    l = jnp.broadcast_to(l, (8, 128))
    l = l + pltpu.roll(l, 2, 0)
    inv = 1.0 / l
    inv = jnp.concatenate([inv, inv], 1)
    o = jnp.zeros((16, 256), F32)
    for j in range(tiles):
        w = p[j] * inv
        w = jnp.concatenate([w, w], 0).astype(BF16)
        va = vbuf[slot, 512 * j : 512 * j + 256, :]
        vb = vbuf[slot, 512 * j + 256 : 512 * j + 512, :]
        o = o + jnp.dot(w, jnp.concatenate([va, vb], 1), preferred_element_type=F32)
    o = o[:8]
    o = o[:, :128] + pltpu.roll(o[:, 128:], 6, 0)
    seen_ref[b] = o


def attention(q_ref, k_ref, v_ref, out_ref, kbuf, vbuf, s_ref, seen_ref, ksem, vsem):
    n = k_ref.shape[0]
    tiles = k_ref.shape[1] // 512

    def kcopy(b, slot):
        return pltpu.make_async_copy(k_ref.at[b], kbuf.at[slot], ksem.at[slot])

    def vcopy(b, slot):
        return pltpu.make_async_copy(v_ref.at[b], vbuf.at[slot], vsem.at[slot])

    for s in range(NK):
        kcopy(s, s).start()
        vcopy(s, s).start()
    kcopy(0, 0).wait()
    scores_of(q_ref, kbuf, s_ref, 0, 0, 0, tiles)
    kcopy(NK, 0).start()

    def body(i, carry):
        kslot, vslot = lax.rem(i + 1, NK), lax.rem(i, NV)
        kcopy(i + 1, kslot).wait()
        vcopy(i, vslot).wait()
        par = lax.rem(i, 2)
        scores_of(q_ref, kbuf, s_ref, i + 1, kslot, 1 - par, tiles)
        seen_from(s_ref, vbuf, seen_ref, i, vslot, par, tiles)

        @pl.when(i + 1 + NK < n)
        def _():
            kcopy(i + 1 + NK, kslot).start()

        @pl.when(i + NV < n)
        def _():
            vcopy(i + NV, vslot).start()

        return carry

    lax.fori_loop(0, n - 1, body, 0)
    vcopy(n - 1, (n - 1) % NV).wait()
    seen_from(s_ref, vbuf, seen_ref, n - 1, (n - 1) % NV, (n - 1) % 2, tiles)
    out_ref[...] = jnp.concatenate([seen_ref[:, 0, :], seen_ref[:, 1, :]], 1).astype(BF16)


def attend(q, k, v):
    n, rows, head = k.shape
    return pl.pallas_call(
        attention,
        out_shape=jax.ShapeDtypeStruct((n, 2 * head), BF16),
        in_specs=[pl.BlockSpec(memory_space=pltpu.VMEM)] + [pl.BlockSpec(memory_space=pl.ANY)] * 2,
        out_specs=pl.BlockSpec(memory_space=pltpu.VMEM),
        scratch_shapes=[
            pltpu.VMEM((NK, rows, head), BF16),
            pltpu.VMEM((NV, rows, head), BF16),
            pltpu.VMEM((2, 8, rows // 2), F32),
            pltpu.VMEM((n, 8, head), F32),
            pltpu.SemaphoreType.DMA((NK,)),
            pltpu.SemaphoreType.DMA((NV,)),
        ],
        compiler_params=pltpu.CompilerParams(vmem_limit_bytes=60 << 20),
    )(q, k, v)


def seen_by(a, wq, k_cache, v_cache, head, theta):
    batch, cache, kv_heads = k_cache.shape[:3]
    place = jnp.full((batch,), cache - 1)
    q = turned(matmul(a, wq).reshape(batch, -1, head), place, theta).reshape(batch, -1)
    return attend(q.astype(F32), k_cache.reshape(batch, -1, head), v_cache.reshape(batch, -1, head))


def solution(mesh):
    def added(t, term):
        return (t.astype(jnp.float32) + lax.psum(term.astype(jnp.bfloat16), "tp").astype(jnp.float32)).astype(jnp.bfloat16)

    def step(x, k_cache, v_cache, gain_a, wq, wo, gain_m, w_gate, w_up, w_down):
        seen = seen_by(normed(x, gain_a), wq, k_cache, v_cache, HEAD, THETA)
        h = added(x, jnp.dot(seen, wo, preferred_element_type=jnp.float32))
        return added(h, jnp.dot(hidden_of(normed(h, gain_m), w_gate, w_up), w_down, preferred_element_type=jnp.float32))

    states, cache, columns, rows_of = P("dp", None), P("dp", None, "tp", None), P(None, "tp"), P("tp", None)
    return jax.shard_map(
        step,
        mesh=mesh,
        in_specs=(states, cache, cache, P(None), columns, rows_of, P(None), columns, columns, rows_of),
        out_specs=states,
        check_vma=False,
    )
```

```python
import functools

import jax
import jax.numpy as jnp
import numpy as np
from jax import lax
from jax.experimental import pallas as pl
from jax.experimental.pallas import tpu as pltpu
from jax.sharding import PartitionSpec as P

HEAD = 128
THETA = 10000
F32, BF16 = jnp.float32, jnp.bfloat16
LOG2E = 1.4426950408889634
NK = NV = 6
G = 8
RS_H, AG_H, RS_Y, AG_Y = range(4)


def normed(wide, gain):
    gain = gain.astype(F32)
    gain = jnp.concatenate([gain[c : c + 1] for c in range(gain.shape[0])], 1)
    scale = lax.rsqrt(jnp.mean(wide * wide, -1, keepdims=True) + 1e-6)
    return (wide * scale * gain).astype(BF16)


def twice(t):
    return jnp.concatenate([t, t], 0).astype(BF16)


def scores_of(q_ref, kbuf, s_ref, b, slot, par):
    row = q_ref[pl.ds(b, 1), :]
    q0 = jnp.broadcast_to(row[:, :HEAD], (16, HEAD))
    q1 = jnp.broadcast_to(row[:, HEAD:], (16, HEAD))
    r = lax.broadcasted_iota(jnp.int32, (16, HEAD), 0)
    q = jnp.where((r & 1) == 0, q0, q1)
    first = (r & 2) == 0
    lhs = jnp.concatenate([jnp.where(first, q, 0.0), jnp.where(first, 0.0, q)], 1).astype(BF16)
    for j in range(kbuf.shape[1] // 512):
        ka = kbuf[slot, 512 * j : 512 * j + 256, :]
        kb = kbuf[slot, 512 * j + 256 : 512 * j + 512, :]
        s = lax.dot_general(lhs, jnp.concatenate([ka, kb], 1), (((1,), (1,)), ((), ())), preferred_element_type=F32)
        s_ref[par, :, 256 * j : 256 * j + 256] = s[:8]


def seen_from(s_ref, vbuf, seen_ref, b, slot, par):
    tiles = vbuf.shape[1] // 512
    r = lax.broadcasted_iota(jnp.int32, (8, 256), 0)
    c = lax.broadcasted_iota(jnp.int32, (8, 256), 1)
    mine = (r & 1) == (c & 1)
    t = [jnp.where(mine, s_ref[par, :, 256 * j : 256 * j + 256], -1e30) for j in range(tiles)]
    m = functools.reduce(jnp.maximum, t)
    m = jnp.max(jnp.maximum(m[:, :128], m[:, 128:]), 1, keepdims=True)
    m = jnp.broadcast_to(m, (8, 128))
    m = jnp.maximum(m, pltpu.roll(m, 2, 0))
    m = jnp.concatenate([m, m], 1)
    k = HEAD**-0.5 * LOG2E
    p = [jnp.exp2((x - m) * k) for x in t]
    l = functools.reduce(jnp.add, p)
    l = jnp.sum(l[:, :128] + l[:, 128:], 1, keepdims=True)
    l = jnp.broadcast_to(l, (8, 128))
    l = l + pltpu.roll(l, 2, 0)
    inv = 1.0 / l
    inv = jnp.concatenate([inv, inv], 1)
    o = jnp.zeros((16, 256), F32)
    for j in range(tiles):
        va = vbuf[slot, 512 * j : 512 * j + 256, :]
        vb = vbuf[slot, 512 * j + 256 : 512 * j + 512, :]
        o = o + jnp.dot(twice(p[j] * inv), jnp.concatenate([va, vb], 1), preferred_element_type=F32)
    o = o[:8]
    seen_ref[b] = o[:, :128] + pltpu.roll(o[:, 128:], 6, 0)


def layer(
    n_dev, x_ref, k_ref, v_ref, ga_ref, wq_ref, wo_ref, gm_ref, wg_ref, wu_ref, wd_ref, turn_ref, out_ref,
    kbuf, vbuf, x_v, xc_v, ga_v, gm_v, turn_v, wq_v, wo_v, wg_v, wu_v, wd_v,
    q_v, s_v, seen_v, own_v, hsend, hrecv, hmine, hfull, ysend, yrecv, ymine,
    ksem, vsem, wsem, outsem, send_sem, recv_sem,
):
    me = lax.axis_index("tp")
    n = k_ref.shape[0]
    groups = n // G
    d = x_ref.shape[2]
    cols = d // n_dev
    mine = pl.ds(pl.multiple_of(me * cols, cols), cols)
    peers = [lax.rem(me + j, n_dev) for j in range(1, n_dev)]
    sources = [lax.rem(me + n_dev - j, n_dev) for j in range(1, n_dev)]

    barrier = pltpu.get_barrier_semaphore()
    for peer in peers:
        pl.semaphore_signal(barrier, inc=1, device_id={"tp": peer}, device_id_type=pl.DeviceIdType.MESH)

    loads = [
        pltpu.make_async_copy(src, dst, wsem.at[i])
        for i, (src, dst) in enumerate(
            [
                (x_ref, x_v),
                (ga_ref, ga_v),
                (turn_ref, turn_v),
                (wq_ref, wq_v),
                (x_ref.at[:, :, mine], xc_v),
                (gm_ref, gm_v),
                (wo_ref, wo_v),
                (wg_ref, wg_v),
                (wu_ref, wu_v),
                (wd_ref, wd_v),
            ]
        )
    ]

    def kcopy(b, slot):
        return pltpu.make_async_copy(k_ref.at[b], kbuf.at[slot], ksem.at[slot])

    def vcopy(b, slot):
        return pltpu.make_async_copy(v_ref.at[b], vbuf.at[slot], vsem.at[slot])

    def scatter(phase, buf, into, peer, source):
        return pltpu.make_async_remote_copy(
            src_ref=buf.at[peer],
            dst_ref=into.at[source],
            send_sem=send_sem.at[phase, peer],
            recv_sem=recv_sem.at[phase, source],
            device_id={"tp": peer},
            device_id_type=pl.DeviceIdType.MESH,
        )

    def gather(phase, chunk, into, peer, source):
        at = pl.ds(pl.multiple_of(source * cols, cols), cols)
        return pltpu.make_async_remote_copy(
            src_ref=chunk,
            dst_ref=into.at[:, at],
            send_sem=send_sem.at[phase, peer],
            recv_sem=recv_sem.at[phase, source],
            device_id={"tp": peer},
            device_id_type=pl.DeviceIdType.MESH,
        )

    def summed(recv, own):
        total = own
        for source in sources:
            total = total + recv[source].astype(F32)
        return total

    def term(g, out, send, recv, phase):
        for i in range(n_dev):
            own_v[i] = out[:G, cols * i : cols * (i + 1)]
            send[i] = out[:G, cols * i : cols * (i + 1)].astype(BF16)
        for peer in peers:
            scatter(phase, send, recv, peer, me).start()

    def arrived(phase, send, recv):
        for source in sources:
            scatter(phase, send, recv, me, source).wait_recv()
        for peer in peers:
            scatter(phase, send, recv, peer, me).wait_send()

    def attended(g):
        @pl.when(g == 0)
        def _():
            loads[6].wait()

        rows = pl.ds(g * G, G)
        seen = jnp.concatenate([seen_v[rows, 0, :], seen_v[rows, 1, :]], 1)
        out = jnp.dot(twice(seen), wo_v[...], preferred_element_type=F32)
        term(g, out, hsend, hrecv, RS_H)

    def half(g):
        arrived(RS_H, hsend, hrecv)
        h = (xc_v[g].astype(F32) + summed(hrecv, own_v[me])).astype(BF16)
        hmine[...] = h
        hfull[:, mine] = h
        for peer in peers:
            gather(AG_H, hmine, hfull, peer, me).start()

    def through(g):
        @pl.when(g == 0)
        def _():
            for load in loads[7:]:
                load.wait()

        for source in sources:
            gather(AG_H, hmine, hfull, me, source).wait_recv()
        for peer in peers:
            gather(AG_H, hmine, hfull, peer, me).wait_send()
        b = twice(normed(hfull[...].astype(F32), gm_v[...]).astype(F32))
        gate = jnp.dot(b, wg_v[...], preferred_element_type=F32)
        up = jnp.dot(b, wu_v[...], preferred_element_type=F32)
        out = jnp.dot((jax.nn.silu(gate) * up).astype(BF16), wd_v[...], preferred_element_type=F32)
        term(g, out, ysend, yrecv, RS_Y)

    def whole(g):
        arrived(RS_Y, ysend, yrecv)
        ymine[...] = (hmine[...].astype(F32) + summed(yrecv, own_v[me])).astype(BF16)
        for peer in peers:
            gather(AG_Y, ymine, out_ref.at[g], peer, me).start()
        pltpu.make_async_copy(ymine, out_ref.at[g, :, mine], outsem).start()

    def done(g):
        for source in sources:
            gather(AG_Y, ymine, out_ref.at[g], me, source).wait_recv()
        for peer in peers:
            gather(AG_Y, ymine, out_ref.at[g], peer, me).wait_send()
        pltpu.make_async_copy(ymine, out_ref.at[g, :, mine], outsem).wait()

    for load in loads[:4]:
        load.start()
    for s in range(NK):
        kcopy(s, s).start()
        vcopy(s, s).start()
    for load in loads[4:]:
        load.start()

    for load in loads[:4]:
        load.wait()
    wide = jnp.concatenate([x_v[g] for g in range(groups)], 0).astype(F32)
    q = jnp.dot(normed(wide, ga_v[...]), wq_v[...], preferred_element_type=F32).astype(BF16).astype(F32)
    for i in range(2):
        t = q[:, HEAD * i : HEAD * (i + 1)]
        t = t * turn_v[0:1, :] + pltpu.roll(t, HEAD // 2, 1) * turn_v[1:2, :]
        q_v[:, HEAD * i : HEAD * (i + 1)] = t.astype(BF16).astype(F32)
    loads[4].wait()
    loads[5].wait()
    pl.semaphore_wait(barrier, n_dev - 1)

    kcopy(0, 0).wait()
    scores_of(q_v, kbuf, s_v, 0, 0, 0)
    kcopy(NK, 0).start()

    def sequence(i, carry):
        kslot, vslot = lax.rem(i + 1, NK), lax.rem(i, NV)
        kcopy(i + 1, kslot).wait()
        vcopy(i, vslot).wait()
        par = lax.rem(i, 2)
        scores_of(q_v, kbuf, s_v, i + 1, kslot, 1 - par)
        seen_from(s_v, vbuf, seen_v, i, vslot, par)

        @pl.when(i + 1 + NK < n)
        def _():
            kcopy(i + 1 + NK, kslot).start()

        @pl.when(i + NV < n)
        def _():
            vcopy(i + NV, vslot).start()

        return carry

    steps = (half, through, whole, done)
    each = G // len(steps)

    def group(g, carry):
        for j, step in enumerate(steps):
            lax.fori_loop(g * G + each * j, g * G + each * (j + 1), sequence, 0)

            @pl.when(g > 0)
            def _():
                step(g - 1)

        attended(g)
        return carry

    lax.fori_loop(0, groups - 1, group, 0)
    g = groups - 1
    for j, step in enumerate(steps):
        lax.fori_loop(g * G + each * j, min(g * G + each * (j + 1), n - 1), sequence, 0)
        step(g - 1)
    vcopy(n - 1, (n - 1) % NV).wait()
    seen_from(s_v, vbuf, seen_v, n - 1, (n - 1) % NV, (n - 1) % 2)
    attended(g)
    for step in steps:
        step(g)


def solution(mesh):
    n_dev = mesh.shape["tp"]

    def step(x, k_cache, v_cache, gain_a, wq, wo, gain_m, w_gate, w_up, w_down):
        n, d = x.shape
        cache = k_cache.shape[1]
        half = HEAD // 2
        angle = np.float32(cache - 1) * np.float32(THETA) ** (-np.arange(half, dtype=np.float32) / np.float32(half))
        angle = angle.astype(np.float32).astype(np.float64)
        cos, sin = np.cos(angle).astype(np.float32), np.sin(angle).astype(np.float32)
        turn = np.stack([np.concatenate([cos, cos]), np.concatenate([-sin, sin])])
        cols, ff = d // n_dev, w_gate.shape[1]
        rows = cache * 2
        out = pl.pallas_call(
            functools.partial(layer, n_dev),
            out_shape=jax.ShapeDtypeStruct((n // G, G, d), BF16),
            in_specs=[pl.BlockSpec(memory_space=pl.ANY)] * 11,
            out_specs=pl.BlockSpec(memory_space=pl.ANY),
            scratch_shapes=[
                pltpu.VMEM((NK, rows, HEAD), BF16),
                pltpu.VMEM((NV, rows, HEAD), BF16),
                pltpu.VMEM((n // G, G, d), BF16),
                pltpu.VMEM((n // G, G, cols), BF16),
                pltpu.VMEM((d // HEAD, HEAD), BF16),
                pltpu.VMEM((d // HEAD, HEAD), BF16),
                pltpu.VMEM((2, HEAD), F32),
                pltpu.VMEM((d, 2 * HEAD), BF16),
                pltpu.VMEM((2 * HEAD, d), BF16),
                pltpu.VMEM((d, ff), BF16),
                pltpu.VMEM((d, ff), BF16),
                pltpu.VMEM((ff, d), BF16),
                pltpu.VMEM((n, 2 * HEAD), F32),
                pltpu.VMEM((2, 8, rows // 2), F32),
                pltpu.VMEM((n, 8, HEAD), F32),
                pltpu.VMEM((n_dev, G, cols), F32),
                pltpu.VMEM((n_dev, G, cols), BF16),
                pltpu.VMEM((n_dev, G, cols), BF16),
                pltpu.VMEM((G, cols), BF16),
                pltpu.VMEM((G, d), BF16),
                pltpu.VMEM((n_dev, G, cols), BF16),
                pltpu.VMEM((n_dev, G, cols), BF16),
                pltpu.VMEM((G, cols), BF16),
                pltpu.SemaphoreType.DMA((NK,)),
                pltpu.SemaphoreType.DMA((NV,)),
                pltpu.SemaphoreType.DMA((10,)),
                pltpu.SemaphoreType.DMA,
                pltpu.SemaphoreType.DMA((4, n_dev)),
                pltpu.SemaphoreType.DMA((4, n_dev)),
            ],
            compiler_params=pltpu.CompilerParams(vmem_limit_bytes=60 << 20, collective_id=0, has_side_effects=True),
        )(
            x.reshape(n // G, G, d),
            k_cache.reshape(n, rows, HEAD),
            v_cache.reshape(n, rows, HEAD),
            gain_a.reshape(-1, HEAD),
            wq,
            wo,
            gain_m.reshape(-1, HEAD),
            w_gate,
            w_up,
            w_down,
            jnp.asarray(turn),
        )
        return out.reshape(n, d)

    states, cache, columns, rows_of = P("dp", None), P("dp", None, "tp", None), P(None, "tp"), P("tp", None)
    return jax.shard_map(
        step,
        mesh=mesh,
        in_specs=(states, cache, cache, P(None), columns, rows_of, P(None), columns, columns, rows_of),
        out_specs=states,
        check_vma=False,
    )
```

```python
import functools

import jax
import jax.numpy as jnp
import numpy as np
from jax import lax
from jax.experimental import pallas as pl
from jax.experimental.pallas import tpu as pltpu
from jax.sharding import PartitionSpec as P

HEAD = 128
THETA = 10000
F32, BF16 = jnp.float32, jnp.bfloat16
LOG2E = 1.4426950408889634
NK = NV = 6
G = 8
RS_H, AG_H, RS_Y, AG_Y = range(4)


def normed(wide, gain):
    gain = gain.astype(F32)
    gain = jnp.concatenate([gain[c : c + 1] for c in range(gain.shape[0])], 1)
    scale = lax.rsqrt(jnp.mean(wide * wide, -1, keepdims=True) + 1e-6)
    return (wide * scale * gain).astype(BF16)


def twice(t):
    return jnp.concatenate([t, t], 0).astype(BF16)


def scores_of(q_ref, kbuf, s_ref, b, slot):
    row = q_ref[pl.ds(b, 1), :]
    q0 = jnp.broadcast_to(row[:, :HEAD], (16, HEAD))
    q1 = jnp.broadcast_to(row[:, HEAD:], (16, HEAD))
    r = lax.broadcasted_iota(jnp.int32, (16, HEAD), 0)
    q = jnp.where((r & 1) == 0, q0, q1)
    first = (r & 2) == 0
    lhs = jnp.concatenate([jnp.where(first, q, 0.0), jnp.where(first, 0.0, q)], 1).astype(BF16)
    for j in range(kbuf.shape[1] // 512):
        ka = kbuf[slot, 512 * j : 512 * j + 256, :]
        kb = kbuf[slot, 512 * j + 256 : 512 * j + 512, :]
        s = lax.dot_general(lhs, jnp.concatenate([ka, kb], 1), (((1,), (1,)), ((), ())), preferred_element_type=F32)
        s_ref[:, 256 * j : 256 * j + 256] = s[:8]


def weights_of(s_ref, p_ref):
    tiles = s_ref.shape[1] // 256
    r = lax.broadcasted_iota(jnp.int32, (8, 256), 0)
    c = lax.broadcasted_iota(jnp.int32, (8, 256), 1)
    mine = (r & 1) == (c & 1)
    t = [jnp.where(mine, s_ref[:, 256 * j : 256 * j + 256], -1e30) for j in range(tiles)]
    m = functools.reduce(jnp.maximum, t)
    m = jnp.max(jnp.maximum(m[:, :128], m[:, 128:]), 1, keepdims=True)
    m = jnp.broadcast_to(m, (8, 128))
    m = jnp.maximum(m, pltpu.roll(m, 2, 0))
    m = jnp.concatenate([m, m], 1)
    k = HEAD**-0.5 * LOG2E
    p = [jnp.exp2((x - m) * k) for x in t]
    l = functools.reduce(jnp.add, p)
    l = jnp.sum(l[:, :128] + l[:, 128:], 1, keepdims=True)
    l = jnp.broadcast_to(l, (8, 128))
    l = l + pltpu.roll(l, 2, 0)
    inv = 1.0 / l
    inv = jnp.concatenate([inv, inv], 1)
    for j in range(tiles):
        p_ref[:, 256 * j : 256 * j + 256] = twice(p[j] * inv)


def seen_from(p_ref, vbuf, seen_ref, b, slot):
    o = jnp.zeros((16, 256), F32)
    for j in range(vbuf.shape[1] // 512):
        va = vbuf[slot, 512 * j : 512 * j + 256, :]
        vb = vbuf[slot, 512 * j + 256 : 512 * j + 512, :]
        o = o + jnp.dot(p_ref[:, 256 * j : 256 * j + 256], jnp.concatenate([va, vb], 1), preferred_element_type=F32)
    o = o[:8]
    seen_ref[b] = o[:, :128] + pltpu.roll(o[:, 128:], 6, 0)


def layer(
    n_dev, x_ref, k_ref, v_ref, ga_ref, wq_ref, wo_ref, gm_ref, wg_ref, wu_ref, wd_ref, turn_ref, out_ref,
    kbuf, vbuf, x_v, xc_v, ga_v, gm_v, turn_v, wq_v, wo_v, wg_v, wu_v, wd_v,
    q_v, s0_v, s1_v, p0_v, p1_v, seen_v, own_v, hsend, hrecv, hmine, hfull, ysend, yrecv, ymine,
    ksem, vsem, wsem, outsem, send_sem, recv_sem,
):
    me = lax.axis_index("tp")
    n = k_ref.shape[0]
    groups = n // G
    d = x_ref.shape[2]
    cols = d // n_dev
    mine = pl.ds(pl.multiple_of(me * cols, cols), cols)
    peers = [lax.rem(me + j, n_dev) for j in range(1, n_dev)]
    sources = [lax.rem(me + n_dev - j, n_dev) for j in range(1, n_dev)]

    barrier = pltpu.get_barrier_semaphore()
    for peer in peers:
        pl.semaphore_signal(barrier, inc=1, device_id={"tp": peer}, device_id_type=pl.DeviceIdType.MESH)

    loads = [
        pltpu.make_async_copy(src, dst, wsem.at[i])
        for i, (src, dst) in enumerate(
            [
                (x_ref, x_v),
                (ga_ref, ga_v),
                (turn_ref, turn_v),
                (wq_ref, wq_v),
                (x_ref.at[:, :, mine], xc_v),
                (gm_ref, gm_v),
                (wo_ref, wo_v),
                (wg_ref, wg_v),
                (wu_ref, wu_v),
                (wd_ref, wd_v),
            ]
        )
    ]

    def kcopy(b, slot):
        return pltpu.make_async_copy(k_ref.at[b], kbuf.at[slot], ksem.at[slot])

    def vcopy(b, slot):
        return pltpu.make_async_copy(v_ref.at[b], vbuf.at[slot], vsem.at[slot])

    def scatter(phase, buf, into, peer, source):
        return pltpu.make_async_remote_copy(
            src_ref=buf.at[peer],
            dst_ref=into.at[source],
            send_sem=send_sem.at[phase, peer],
            recv_sem=recv_sem.at[phase, source],
            device_id={"tp": peer},
            device_id_type=pl.DeviceIdType.MESH,
        )

    def gather(phase, chunk, into, peer, source):
        at = pl.ds(pl.multiple_of(source * cols, cols), cols)
        return pltpu.make_async_remote_copy(
            src_ref=chunk,
            dst_ref=into.at[:, at],
            send_sem=send_sem.at[phase, peer],
            recv_sem=recv_sem.at[phase, source],
            device_id={"tp": peer},
            device_id_type=pl.DeviceIdType.MESH,
        )

    def summed(recv, own):
        total = own
        for source in sources:
            total = total + recv[source].astype(F32)
        return total

    def term(g, out, send, recv, phase):
        for i in range(n_dev):
            own_v[i] = out[:G, cols * i : cols * (i + 1)]
            send[i] = out[:G, cols * i : cols * (i + 1)].astype(BF16)
        for peer in peers:
            scatter(phase, send, recv, peer, me).start()

    def arrived(phase, send, recv):
        for source in sources:
            scatter(phase, send, recv, me, source).wait_recv()
        for peer in peers:
            scatter(phase, send, recv, peer, me).wait_send()

    def attended(g):
        @pl.when(g == 0)
        def _():
            loads[6].wait()

        rows = pl.ds(g * G, G)
        seen = jnp.concatenate([seen_v[rows, 0, :], seen_v[rows, 1, :]], 1)
        out = jnp.dot(twice(seen), wo_v[...], preferred_element_type=F32)
        term(g, out, hsend, hrecv, RS_H)

    def half(g):
        arrived(RS_H, hsend, hrecv)
        h = (xc_v[g].astype(F32) + summed(hrecv, own_v[me])).astype(BF16)
        hmine[...] = h
        hfull[:, mine] = h
        for peer in peers:
            gather(AG_H, hmine, hfull, peer, me).start()

    def through(g):
        @pl.when(g == 0)
        def _():
            for load in loads[7:]:
                load.wait()

        for source in sources:
            gather(AG_H, hmine, hfull, me, source).wait_recv()
        for peer in peers:
            gather(AG_H, hmine, hfull, peer, me).wait_send()
        b = twice(normed(hfull[...].astype(F32), gm_v[...]).astype(F32))
        gate = jnp.dot(b, wg_v[...], preferred_element_type=F32)
        up = jnp.dot(b, wu_v[...], preferred_element_type=F32)
        out = jnp.dot((jax.nn.silu(gate) * up).astype(BF16), wd_v[...], preferred_element_type=F32)
        term(g, out, ysend, yrecv, RS_Y)

    def whole(g):
        arrived(RS_Y, ysend, yrecv)
        ymine[...] = (hmine[...].astype(F32) + summed(yrecv, own_v[me])).astype(BF16)
        for peer in peers:
            gather(AG_Y, ymine, out_ref.at[g], peer, me).start()
        pltpu.make_async_copy(ymine, out_ref.at[g, :, mine], outsem).start()

    def done(g):
        for source in sources:
            gather(AG_Y, ymine, out_ref.at[g], me, source).wait_recv()
        for peer in peers:
            gather(AG_Y, ymine, out_ref.at[g], peer, me).wait_send()
        pltpu.make_async_copy(ymine, out_ref.at[g, :, mine], outsem).wait()

    for load in loads[:4]:
        load.start()
    for s in range(NK):
        kcopy(s, s).start()
        vcopy(s, s).start()
    for load in loads[4:]:
        load.start()

    for load in loads[:4]:
        load.wait()
    wide = jnp.concatenate([x_v[g] for g in range(groups)], 0).astype(F32)
    q = jnp.dot(normed(wide, ga_v[...]), wq_v[...], preferred_element_type=F32).astype(BF16).astype(F32)
    for i in range(2):
        t = q[:, HEAD * i : HEAD * (i + 1)]
        t = t * turn_v[0:1, :] + pltpu.roll(t, HEAD // 2, 1) * turn_v[1:2, :]
        q_v[:, HEAD * i : HEAD * (i + 1)] = t.astype(BF16).astype(F32)
    loads[4].wait()
    loads[5].wait()
    pl.semaphore_wait(barrier, n_dev - 1)

    score, weight = (s0_v, s1_v), (p0_v, p1_v)
    for b in range(2):
        kcopy(b, b).wait()
        scores_of(q_v, kbuf, score[b], b, b)
        kcopy(b + NK, b).start()

    def pair(p, carry):
        i = 2 * p
        for b in range(2):
            kcopy(i + b + 2, lax.rem(i + b + 2, NK)).wait()
            vcopy(i + b, lax.rem(i + b, NV)).wait()
        for b in range(2):
            weights_of(score[b], weight[b])
        for b in range(2):
            scores_of(q_v, kbuf, score[b], i + b + 2, lax.rem(i + b + 2, NK))
        for b in range(2):
            seen_from(weight[b], vbuf, seen_v, i + b, lax.rem(i + b, NV))

        @pl.when(i + 2 + NK < n)
        def _():
            for b in range(2):
                kcopy(i + b + 2 + NK, lax.rem(i + b + 2, NK)).start()

        @pl.when(i + NV < n)
        def _():
            for b in range(2):
                vcopy(i + b + NV, lax.rem(i + b, NV)).start()

        g, j = p // pairs, lax.rem(p, pairs)
        for at, step in enumerate(steps):

            @pl.when((j == at) & (g > 0))
            def _():
                step(g - 1)

        @pl.when(j == pairs - 1)
        def _():
            attended(g)

        return carry

    steps = (half, through, whole, done)
    pairs = G // 2
    lax.fori_loop(0, n // 2 - 1, pair, 0)
    for b in range(2):
        weights_of(score[b], weight[b])
    for b in range(n - 2, n):
        vcopy(b, b % NV).wait()
        seen_from(weight[b % 2], vbuf, seen_v, b, b % NV)
    g = groups - 1
    done(g - 1)
    attended(g)
    for step in steps:
        step(g)


def solution(mesh):
    n_dev = mesh.shape["tp"]

    def step(x, k_cache, v_cache, gain_a, wq, wo, gain_m, w_gate, w_up, w_down):
        n, d = x.shape
        cache = k_cache.shape[1]
        half = HEAD // 2
        angle = np.float32(cache - 1) * np.float32(THETA) ** (-np.arange(half, dtype=np.float32) / np.float32(half))
        angle = angle.astype(np.float32).astype(np.float64)
        cos, sin = np.cos(angle).astype(np.float32), np.sin(angle).astype(np.float32)
        turn = np.stack([np.concatenate([cos, cos]), np.concatenate([-sin, sin])])
        cols, ff = d // n_dev, w_gate.shape[1]
        rows = cache * 2
        out = pl.pallas_call(
            functools.partial(layer, n_dev),
            out_shape=jax.ShapeDtypeStruct((n // G, G, d), BF16),
            in_specs=[pl.BlockSpec(memory_space=pl.ANY)] * 11,
            out_specs=pl.BlockSpec(memory_space=pl.ANY),
            scratch_shapes=[
                pltpu.VMEM((NK, rows, HEAD), BF16),
                pltpu.VMEM((NV, rows, HEAD), BF16),
                pltpu.VMEM((n // G, G, d), BF16),
                pltpu.VMEM((n // G, G, cols), BF16),
                pltpu.VMEM((d // HEAD, HEAD), BF16),
                pltpu.VMEM((d // HEAD, HEAD), BF16),
                pltpu.VMEM((2, HEAD), F32),
                pltpu.VMEM((d, 2 * HEAD), BF16),
                pltpu.VMEM((2 * HEAD, d), BF16),
                pltpu.VMEM((d, ff), BF16),
                pltpu.VMEM((d, ff), BF16),
                pltpu.VMEM((ff, d), BF16),
                pltpu.VMEM((n, 2 * HEAD), F32),
                pltpu.VMEM((8, rows // 2), F32),
                pltpu.VMEM((8, rows // 2), F32),
                pltpu.VMEM((16, rows // 2), BF16),
                pltpu.VMEM((16, rows // 2), BF16),
                pltpu.VMEM((n, 8, HEAD), F32),
                pltpu.VMEM((n_dev, G, cols), F32),
                pltpu.VMEM((n_dev, G, cols), BF16),
                pltpu.VMEM((n_dev, G, cols), BF16),
                pltpu.VMEM((G, cols), BF16),
                pltpu.VMEM((G, d), BF16),
                pltpu.VMEM((n_dev, G, cols), BF16),
                pltpu.VMEM((n_dev, G, cols), BF16),
                pltpu.VMEM((G, cols), BF16),
                pltpu.SemaphoreType.DMA((NK,)),
                pltpu.SemaphoreType.DMA((NV,)),
                pltpu.SemaphoreType.DMA((10,)),
                pltpu.SemaphoreType.DMA,
                pltpu.SemaphoreType.DMA((4, n_dev)),
                pltpu.SemaphoreType.DMA((4, n_dev)),
            ],
            compiler_params=pltpu.CompilerParams(vmem_limit_bytes=60 << 20, collective_id=0, has_side_effects=True),
        )(
            x.reshape(n // G, G, d),
            k_cache.reshape(n, rows, HEAD),
            v_cache.reshape(n, rows, HEAD),
            gain_a.reshape(-1, HEAD),
            wq,
            wo,
            gain_m.reshape(-1, HEAD),
            w_gate,
            w_up,
            w_down,
            jnp.asarray(turn),
        )
        return out.reshape(n, d)

    states, cache, columns, rows_of = P("dp", None), P("dp", None, "tp", None), P(None, "tp"), P("tp", None)
    return jax.shard_map(
        step,
        mesh=mesh,
        in_specs=(states, cache, cache, P(None), columns, rows_of, P(None), columns, columns, rows_of),
        out_specs=states,
        check_vma=False,
    )
```

```python
import functools

import jax
import jax.numpy as jnp
import numpy as np
from jax import lax
from jax.experimental import pallas as pl
from jax.experimental.pallas import tpu as pltpu
from jax.sharding import PartitionSpec as P

HEAD = 128
THETA = 10000
F32, BF16 = jnp.float32, jnp.bfloat16
LOG2E = 1.4426950408889634
BLOCK = 8
NK = NV = 6
GROUPS = [
    (0, 16, 7, 11, 15),
    (16, 16, 15, 19, 23),
    (32, 16, 23, 27, 29),
    (48, 8, 27, 30, 34),
    (56, 4, 29, 33, 36),
    (60, 4, 32, 35, 37),
]


def normed(wide, gain):
    gain = gain.astype(F32)
    gain = jnp.concatenate([gain[c : c + 1] for c in range(gain.shape[0])], 1)
    scale = lax.rsqrt(jnp.mean(wide * wide, -1, keepdims=True) + 1e-6)
    return (wide * scale * gain).astype(BF16)


def twice(t):
    return jnp.concatenate([t, t], 0).astype(BF16)


def scores_of(q_ref, kbuf, s_ref, b, slot):
    row = q_ref[pl.ds(b, 1), :]
    q0 = jnp.broadcast_to(row[:, :HEAD], (16, HEAD))
    q1 = jnp.broadcast_to(row[:, HEAD:], (16, HEAD))
    r = lax.broadcasted_iota(jnp.int32, (16, HEAD), 0)
    q = jnp.where((r & 1) == 0, q0, q1)
    first = (r & 2) == 0
    lhs = jnp.concatenate([jnp.where(first, q, 0.0), jnp.where(first, 0.0, q)], 1).astype(BF16)
    for j in range(kbuf.shape[1] // 512):
        ka = kbuf[slot, 512 * j : 512 * j + 256, :]
        kb = kbuf[slot, 512 * j + 256 : 512 * j + 512, :]
        s = lax.dot_general(lhs, jnp.concatenate([ka, kb], 1), (((1,), (1,)), ((), ())), preferred_element_type=F32)
        s_ref[:, 256 * j : 256 * j + 256] = s[:8]


def weights_of(s_ref, p_ref):
    tiles = s_ref.shape[1] // 256
    r = lax.broadcasted_iota(jnp.int32, (8, 256), 0)
    c = lax.broadcasted_iota(jnp.int32, (8, 256), 1)
    mine = (r & 1) == (c & 1)
    t = [jnp.where(mine, s_ref[:, 256 * j : 256 * j + 256], -1e30) for j in range(tiles)]
    m = functools.reduce(jnp.maximum, t)
    m = jnp.max(jnp.maximum(m[:, :128], m[:, 128:]), 1, keepdims=True)
    m = jnp.broadcast_to(m, (8, 128))
    m = jnp.maximum(m, pltpu.roll(m, 2, 0))
    m = jnp.concatenate([m, m], 1)
    k = HEAD**-0.5 * LOG2E
    p = [jnp.exp2((x - m) * k) for x in t]
    l = functools.reduce(jnp.add, p)
    l = jnp.sum(l[:, :128] + l[:, 128:], 1, keepdims=True)
    l = jnp.broadcast_to(l, (8, 128))
    l = l + pltpu.roll(l, 2, 0)
    inv = 1.0 / l
    inv = jnp.concatenate([inv, inv], 1)
    for j in range(tiles):
        p_ref[:, 256 * j : 256 * j + 256] = twice(p[j] * inv)


def seen_from(p_ref, vbuf, seen_ref, b, slot):
    o = jnp.zeros((16, 256), F32)
    for j in range(vbuf.shape[1] // 512):
        va = vbuf[slot, 512 * j : 512 * j + 256, :]
        vb = vbuf[slot, 512 * j + 256 : 512 * j + 512, :]
        o = o + jnp.dot(p_ref[:, 256 * j : 256 * j + 256], jnp.concatenate([va, vb], 1), preferred_element_type=F32)
    o = o[:8]
    seen_ref[b] = o[:, :128] + pltpu.roll(o[:, 128:], 6, 0)


def layer(
    n_dev, x_ref, k_ref, v_ref, ga_ref, wq_ref, wo_ref, gm_ref, wg_ref, wu_ref, wd_ref, turn_ref, out_ref,
    kbuf, vbuf, x_v, ga_v, gm_v, turn_v, wq_v, wo_v, wg_v, wu_v, wd_v,
    q_v, s0_v, s1_v, p0_v, p1_v, seen_v, y_v, *rest,
):
    n_groups = len(GROUPS)
    h_v, hterm, yterm = rest[:n_groups], rest[n_groups : 2 * n_groups], rest[2 * n_groups : 3 * n_groups]
    ksem, vsem, wsem, outsem, send_sem, recv_sem = rest[3 * n_groups :]
    me = lax.axis_index("tp")
    n = k_ref.shape[0]
    block = x_ref.shape[1]
    peers = [lax.rem(me + j, n_dev) for j in range(1, n_dev)]

    barrier = pltpu.get_barrier_semaphore()
    for peer in peers:
        pl.semaphore_signal(barrier, inc=1, device_id={"tp": peer}, device_id_type=pl.DeviceIdType.MESH)

    loads = [
        pltpu.make_async_copy(src, dst, wsem.at[i])
        for i, (src, dst) in enumerate(
            [
                (x_ref, x_v),
                (ga_ref, ga_v),
                (turn_ref, turn_v),
                (wq_ref, wq_v),
                (gm_ref, gm_v),
                (wo_ref, wo_v),
                (wg_ref, wg_v),
                (wu_ref, wu_v),
                (wd_ref, wd_v),
            ]
        )
    ]

    def kcopy(b, slot):
        return pltpu.make_async_copy(k_ref.at[b], kbuf.at[slot], ksem.at[slot])

    def vcopy(b, slot):
        return pltpu.make_async_copy(v_ref.at[b], vbuf.at[slot], vsem.at[slot])

    def rows_of(ref, g):
        first, count = GROUPS[g][:2]
        if count >= block:
            return jnp.concatenate([ref[b] for b in range(first // block, (first + count) // block)], 0)
        return ref[first // block, first % block : first % block + count, :]

    def exchange(g, phase, terms, peer, source):
        return pltpu.make_async_remote_copy(
            src_ref=terms.at[source],
            dst_ref=terms.at[source],
            send_sem=send_sem.at[g, phase, peer],
            recv_sem=recv_sem.at[g, phase, source],
            device_id={"tp": peer},
            device_id_type=pl.DeviceIdType.MESH,
        )

    def send(g, phase, terms, out):
        terms[me] = out[: GROUPS[g][1]].astype(BF16)
        for peer in peers:
            exchange(g, phase, terms, peer, me).start()

    def summed(g, phase, terms):
        for source in peers:
            exchange(g, phase, terms, me, source).wait_recv()
        for peer in peers:
            exchange(g, phase, terms, peer, me).wait_send()
        return functools.reduce(jnp.add, [terms[i].astype(F32) for i in range(n_dev)])

    def filled(t):
        return jnp.concatenate([t] * (16 // t.shape[0]), 0).astype(BF16)

    def attended(g):
        if g == 0:
            loads[5].wait()
        first, count = GROUPS[g][:2]
        seen = jnp.concatenate([seen_v[first : first + count, 0, :], seen_v[first : first + count, 1, :]], 1)
        send(g, 0, hterm[g], jnp.dot(filled(seen), wo_v[...], preferred_element_type=F32))

    def through(g):
        if g == 0:
            for load in (loads[4], *loads[6:]):
                load.wait()
        h = (rows_of(x_v, g).astype(F32) + summed(g, 0, hterm[g])).astype(BF16)
        h_v[g][...] = h
        b = filled(normed(h.astype(F32), gm_v[...]).astype(F32))
        gate = jnp.dot(b, wg_v[...], preferred_element_type=F32)
        up = jnp.dot(b, wu_v[...], preferred_element_type=F32)
        send(g, 1, yterm[g], jnp.dot((jax.nn.silu(gate) * up).astype(BF16), wd_v[...], preferred_element_type=F32))

    def out_copy(b):
        return pltpu.make_async_copy(y_v.at[b], out_ref.at[b], outsem.at[b])

    def done(g):
        first, count = GROUPS[g][:2]
        y = (h_v[g][...].astype(F32) + summed(g, 1, yterm[g])).astype(BF16)
        if count >= block:
            for b in range(count // block):
                y_v[first // block + b] = y[b * block : (b + 1) * block]
        else:
            y_v[first // block, first % block : first % block + count, :] = y
        if (first + count) % block == 0:
            for b in range(first // block, (first + count) // block):
                out_copy(b).start()

    for load in loads[:4]:
        load.start()
    for s in range(NK):
        kcopy(s, s).start()
        vcopy(s, s).start()
    for load in loads[4:]:
        load.start()

    for load in loads[:4]:
        load.wait()
    wide = jnp.concatenate([x_v[b] for b in range(n // block)], 0).astype(F32)
    q = jnp.dot(normed(wide, ga_v[...]), wq_v[...], preferred_element_type=F32).astype(BF16).astype(F32)
    for i in range(2):
        t = q[:, HEAD * i : HEAD * (i + 1)]
        t = t * turn_v[0:1, :] + pltpu.roll(t, HEAD // 2, 1) * turn_v[1:2, :]
        q_v[:, HEAD * i : HEAD * (i + 1)] = t.astype(BF16).astype(F32)
    pl.semaphore_wait(barrier, n_dev - 1)

    score, weight = (s0_v, s1_v), (p0_v, p1_v)
    for b in range(2):
        kcopy(b, b).wait()
        scores_of(q_v, kbuf, score[b], b, b)
        kcopy(b + NK, b).start()

    steps = sorted((at, order, step, g) for g in range(n_groups) for order, (step, at) in enumerate(zip((attended, through, done), GROUPS[g][2:])))

    def pair(p, carry):
        i = 2 * p
        for b in range(2):
            kcopy(i + b + 2, lax.rem(i + b + 2, NK)).wait()
            vcopy(i + b, lax.rem(i + b, NV)).wait()
        for b in range(2):
            weights_of(score[b], weight[b])
        for b in range(2):
            scores_of(q_v, kbuf, score[b], i + b + 2, lax.rem(i + b + 2, NK))
        for b in range(2):
            seen_from(weight[b], vbuf, seen_v, i + b, lax.rem(i + b, NV))

        @pl.when(i + 2 + NK < n)
        def _():
            for b in range(2):
                kcopy(i + b + 2 + NK, lax.rem(i + b + 2, NK)).start()

        @pl.when(i + NV < n)
        def _():
            for b in range(2):
                vcopy(i + b + NV, lax.rem(i + b, NV)).start()

        for at, _, step, g in steps:
            if at < n // 2 - 1:

                @pl.when(p == at)
                def _():
                    step(g)

        return carry

    lax.fori_loop(0, n // 2 - 1, pair, 0)
    for b in range(2):
        weights_of(score[b], weight[b])
    for b in range(n - 2, n):
        vcopy(b, b % NV).wait()
        seen_from(weight[b % 2], vbuf, seen_v, b, b % NV)
    for at, _, step, g in steps:
        if at >= n // 2 - 1:
            step(g)
    for b in range(n // block):
        out_copy(b).wait()


def solution(mesh):
    n_dev = mesh.shape["tp"]

    def step(x, k_cache, v_cache, gain_a, wq, wo, gain_m, w_gate, w_up, w_down):
        n, d = x.shape
        cache = k_cache.shape[1]
        half = HEAD // 2
        angle = np.float32(cache - 1) * np.float32(THETA) ** (-np.arange(half, dtype=np.float32) / np.float32(half))
        angle = angle.astype(np.float32).astype(np.float64)
        cos, sin = np.cos(angle).astype(np.float32), np.sin(angle).astype(np.float32)
        turn = np.stack([np.concatenate([cos, cos]), np.concatenate([-sin, sin])])
        ff = w_gate.shape[1]
        rows = cache * 2
        out = pl.pallas_call(
            functools.partial(layer, n_dev),
            out_shape=jax.ShapeDtypeStruct((n // BLOCK, BLOCK, d), BF16),
            in_specs=[pl.BlockSpec(memory_space=pl.ANY)] * 11,
            out_specs=pl.BlockSpec(memory_space=pl.ANY),
            scratch_shapes=[
                pltpu.VMEM((NK, rows, HEAD), BF16),
                pltpu.VMEM((NV, rows, HEAD), BF16),
                pltpu.VMEM((n // BLOCK, BLOCK, d), BF16),
                pltpu.VMEM((d // HEAD, HEAD), BF16),
                pltpu.VMEM((d // HEAD, HEAD), BF16),
                pltpu.VMEM((2, HEAD), F32),
                pltpu.VMEM((d, 2 * HEAD), BF16),
                pltpu.VMEM((2 * HEAD, d), BF16),
                pltpu.VMEM((d, ff), BF16),
                pltpu.VMEM((d, ff), BF16),
                pltpu.VMEM((ff, d), BF16),
                pltpu.VMEM((n, 2 * HEAD), F32),
                pltpu.VMEM((8, rows // 2), F32),
                pltpu.VMEM((8, rows // 2), F32),
                pltpu.VMEM((16, rows // 2), BF16),
                pltpu.VMEM((16, rows // 2), BF16),
                pltpu.VMEM((n, 8, HEAD), F32),
                pltpu.VMEM((n // BLOCK, BLOCK, d), BF16),
                *[pltpu.VMEM((g[1], d), BF16) for g in GROUPS],
                *[pltpu.VMEM((n_dev, g[1], d), BF16) for g in GROUPS],
                *[pltpu.VMEM((n_dev, g[1], d), BF16) for g in GROUPS],
                pltpu.SemaphoreType.DMA((NK,)),
                pltpu.SemaphoreType.DMA((NV,)),
                pltpu.SemaphoreType.DMA((9,)),
                pltpu.SemaphoreType.DMA((n // BLOCK,)),
                pltpu.SemaphoreType.DMA((len(GROUPS), 2, n_dev)),
                pltpu.SemaphoreType.DMA((len(GROUPS), 2, n_dev)),
            ],
            compiler_params=pltpu.CompilerParams(vmem_limit_bytes=60 << 20, collective_id=0, has_side_effects=True),
        )(
            x.reshape(n // BLOCK, BLOCK, d),
            k_cache.reshape(n, rows, HEAD),
            v_cache.reshape(n, rows, HEAD),
            gain_a.reshape(-1, HEAD),
            wq,
            wo,
            gain_m.reshape(-1, HEAD),
            w_gate,
            w_up,
            w_down,
            jnp.asarray(turn),
        )
        return out.reshape(n, d)

    states, cache, columns, rows_of = P("dp", None), P("dp", None, "tp", None), P(None, "tp"), P("tp", None)
    return jax.shard_map(
        step,
        mesh=mesh,
        in_specs=(states, cache, cache, P(None), columns, rows_of, P(None), columns, columns, rows_of),
        out_specs=states,
        check_vma=False,
    )
```

```python
import functools

import jax
import jax.numpy as jnp
import numpy as np
from jax import lax
from jax.experimental import pallas as pl
from jax.experimental.pallas import tpu as pltpu
from jax.sharding import PartitionSpec as P

HEAD = 128
THETA = 10000
F32, BF16 = jnp.float32, jnp.bfloat16
LOG2E = 1.4426950408889634
BLOCK = 8
NK = NV = 8
GROUPS = [(0, 16), (16, 16), (32, 16), (48, 8), (56, 4), (60, 4)]
STREAM = {
    7: [("attended", 0)],
    11: [("through", 0)],
    15: [("attended", 1), ("done", 0)],
    19: [("through", 1)],
    23: [("attended", 2), ("done", 1)],
    26: [("through", 2)],
    27: [("attended", 3)],
    29: [("attended", 4)],
}
TAIL = [("attended", 5), ("through", 3, 4), ("done", 2), ("through", 5), ("done", 3), ("done", 4), ("done", 5)]


def normed(wide, gain):
    gain = gain.astype(F32)
    gain = jnp.concatenate([gain[c : c + 1] for c in range(gain.shape[0])], 1)
    scale = lax.rsqrt(jnp.mean(wide * wide, -1, keepdims=True) + 1e-6)
    return (wide * scale * gain).astype(BF16)


def twice(t):
    return jnp.concatenate([t, t], 0).astype(BF16)


def scores_of(q_ref, kbuf, s_ref, b, slot):
    row = q_ref[pl.ds(b, 1), :]
    q0 = jnp.broadcast_to(row[:, :HEAD], (16, HEAD))
    q1 = jnp.broadcast_to(row[:, HEAD:], (16, HEAD))
    r = lax.broadcasted_iota(jnp.int32, (16, HEAD), 0)
    q = jnp.where((r & 1) == 0, q0, q1)
    first = (r & 2) == 0
    lhs = jnp.concatenate([jnp.where(first, q, 0.0), jnp.where(first, 0.0, q)], 1).astype(BF16)
    for j in range(kbuf.shape[1] // 512):
        ka = kbuf[slot, 512 * j : 512 * j + 256, :]
        kb = kbuf[slot, 512 * j + 256 : 512 * j + 512, :]
        s = lax.dot_general(lhs, jnp.concatenate([ka, kb], 1), (((1,), (1,)), ((), ())), preferred_element_type=F32)
        s_ref[:, 256 * j : 256 * j + 256] = s[:8]


def weights_of(s_ref, p_ref):
    tiles = s_ref.shape[1] // 256
    r = lax.broadcasted_iota(jnp.int32, (8, 256), 0)
    c = lax.broadcasted_iota(jnp.int32, (8, 256), 1)
    mine = (r & 1) == (c & 1)
    t = [jnp.where(mine, s_ref[:, 256 * j : 256 * j + 256], -1e30) for j in range(tiles)]
    m = functools.reduce(jnp.maximum, t)
    m = jnp.max(jnp.maximum(m[:, :128], m[:, 128:]), 1, keepdims=True)
    m = jnp.broadcast_to(m, (8, 128))
    m = jnp.maximum(m, pltpu.roll(m, 2, 0))
    m = jnp.concatenate([m, m], 1)
    k = HEAD**-0.5 * LOG2E
    p = [jnp.exp2((x - m) * k) for x in t]
    l = functools.reduce(jnp.add, p)
    l = jnp.sum(l[:, :128] + l[:, 128:], 1, keepdims=True)
    l = jnp.broadcast_to(l, (8, 128))
    l = l + pltpu.roll(l, 2, 0)
    inv = 1.0 / l
    inv = jnp.concatenate([inv, inv], 1)
    for j in range(tiles):
        p_ref[:, 256 * j : 256 * j + 256] = twice(p[j] * inv)


def seen_from(p_ref, vbuf, seen_ref, b, slot):
    o = jnp.zeros((16, 256), F32)
    for j in range(vbuf.shape[1] // 512):
        va = vbuf[slot, 512 * j : 512 * j + 256, :]
        vb = vbuf[slot, 512 * j + 256 : 512 * j + 512, :]
        o = o + jnp.dot(p_ref[:, 256 * j : 256 * j + 256], jnp.concatenate([va, vb], 1), preferred_element_type=F32)
    o = o[:8]
    seen_ref[b] = o[:, :128] + pltpu.roll(o[:, 128:], 6, 0)


def layer(
    n_dev, x_ref, k_ref, v_ref, ga_ref, wq_ref, wo_ref, gm_ref, wg_ref, wu_ref, wd_ref, turn_ref, out_ref,
    kbuf, vbuf, x_v, ga_v, gm_v, turn_v, wq_v, wo_v, wg_v, wu_v, wd_v,
    q_v, s0_v, s1_v, p0_v, p1_v, seen_v, *rest,
):
    n_groups = len(GROUPS)
    h_v, hterm, yterm = rest[:n_groups], rest[n_groups : 2 * n_groups], rest[2 * n_groups : 3 * n_groups]
    ksem, vsem, wsem, send_sem, recv_sem = rest[3 * n_groups :]
    me = lax.axis_index("tp")
    n = k_ref.shape[0]
    block = x_ref.shape[1]
    peers = [lax.rem(me + j, n_dev) for j in range(1, n_dev)]

    barrier = pltpu.get_barrier_semaphore()
    for peer in peers:
        pl.semaphore_signal(barrier, inc=1, device_id={"tp": peer}, device_id_type=pl.DeviceIdType.MESH)

    loads = [
        pltpu.make_async_copy(src, dst, wsem.at[i])
        for i, (src, dst) in enumerate(
            [
                (x_ref, x_v),
                (ga_ref, ga_v),
                (turn_ref, turn_v),
                (wq_ref, wq_v),
                (gm_ref, gm_v),
                (wo_ref, wo_v),
                (wg_ref, wg_v),
                (wu_ref, wu_v),
                (wd_ref, wd_v),
            ]
        )
    ]

    def kcopy(b, slot):
        return pltpu.make_async_copy(k_ref.at[b], kbuf.at[slot], ksem.at[slot])

    def vcopy(b, slot):
        return pltpu.make_async_copy(v_ref.at[b], vbuf.at[slot], vsem.at[slot])

    def rows_of(ref, g):
        first, count = GROUPS[g]
        if count >= block:
            return jnp.concatenate([ref[b] for b in range(first // block, (first + count) // block)], 0)
        return ref[first // block, first % block : first % block + count, :]

    def exchange(g, phase, terms, peer, source):
        return pltpu.make_async_remote_copy(
            src_ref=terms.at[source],
            dst_ref=terms.at[source],
            send_sem=send_sem.at[g, phase, peer],
            recv_sem=recv_sem.at[g, phase, source],
            device_id={"tp": peer},
            device_id_type=pl.DeviceIdType.MESH,
        )

    def send(g, phase, terms, out):
        terms[me] = out[: GROUPS[g][1]].astype(BF16)
        for peer in peers:
            exchange(g, phase, terms, peer, me).start()

    def summed(g, phase, terms):
        for source in peers:
            exchange(g, phase, terms, me, source).wait_recv()
        for peer in peers:
            exchange(g, phase, terms, peer, me).wait_send()
        return functools.reduce(jnp.add, [terms[i].astype(F32) for i in range(n_dev)])

    def filled(*parts):
        parts = list(parts)
        while sum(t.shape[0] for t in parts) < 16:
            parts.append(parts[-1])
        return jnp.concatenate(parts, 0).astype(BF16)

    def attended(g):
        if g == 0:
            loads[5].wait()
        first, count = GROUPS[g]
        seen = jnp.concatenate([seen_v[first : first + count, 0, :], seen_v[first : first + count, 1, :]], 1)
        send(g, 0, hterm[g], jnp.dot(filled(seen), wo_v[...], preferred_element_type=F32))

    def through(*gs):
        if 0 in gs:
            for load in (loads[4], *loads[6:]):
                load.wait()
        b = []
        for g in gs:
            h = (rows_of(x_v, g).astype(F32) + summed(g, 0, hterm[g])).astype(BF16)
            h_v[g][...] = h
            b.append(normed(h.astype(F32), gm_v[...]).astype(F32))
        b = filled(*b)
        gate = jnp.dot(b, wg_v[...], preferred_element_type=F32)
        up = jnp.dot(b, wu_v[...], preferred_element_type=F32)
        out = jnp.dot((jax.nn.silu(gate) * up).astype(BF16), wd_v[...], preferred_element_type=F32)
        at = 0
        for g in gs:
            count = GROUPS[g][1]
            send(g, 1, yterm[g], out[at : at + count])
            at += count

    def done(g):
        first, count = GROUPS[g]
        y = (h_v[g][...].astype(F32) + summed(g, 1, yterm[g])).astype(BF16)
        if count >= block:
            for b in range(count // block):
                out_ref[first // block + b] = y[b * block : (b + 1) * block]
        else:
            out_ref[first // block, first % block : first % block + count, :] = y

    named = {"attended": attended, "through": through, "done": done}

    for load in loads[:4]:
        load.start()
    for s in range(NK):
        kcopy(s, s).start()
        vcopy(s, s).start()
    for load in loads[4:]:
        load.start()

    for load in loads[:4]:
        load.wait()
    wide = jnp.concatenate([x_v[b] for b in range(n // block)], 0).astype(F32)
    q = jnp.dot(normed(wide, ga_v[...]), wq_v[...], preferred_element_type=F32).astype(BF16).astype(F32)
    for i in range(2):
        t = q[:, HEAD * i : HEAD * (i + 1)]
        t = t * turn_v[0:1, :] + pltpu.roll(t, HEAD // 2, 1) * turn_v[1:2, :]
        q_v[:, HEAD * i : HEAD * (i + 1)] = t.astype(BF16).astype(F32)
    pl.semaphore_wait(barrier, n_dev - 1)

    score, weight = (s0_v, s1_v), (p0_v, p1_v)
    for b in range(2):
        kcopy(b, b).wait()
        scores_of(q_v, kbuf, score[b], b, b)
        kcopy(b + NK, b).start()

    def pair(p, carry):
        i = 2 * p
        for b in range(2):
            kcopy(i + b + 2, lax.rem(i + b + 2, NK)).wait()
            vcopy(i + b, lax.rem(i + b, NV)).wait()
        for b in range(2):
            weights_of(score[b], weight[b])
        for b in range(2):
            scores_of(q_v, kbuf, score[b], i + b + 2, lax.rem(i + b + 2, NK))
        for b in range(2):
            seen_from(weight[b], vbuf, seen_v, i + b, lax.rem(i + b, NV))

        @pl.when(i + 2 + NK < n)
        def _():
            for b in range(2):
                kcopy(i + b + 2 + NK, lax.rem(i + b + 2, NK)).start()

        @pl.when(i + NV < n)
        def _():
            for b in range(2):
                vcopy(i + b + NV, lax.rem(i + b, NV)).start()

        for at, steps in STREAM.items():

            @pl.when(p == at)
            def _():
                for step, *gs in steps:
                    named[step](*gs)

        return carry

    lax.fori_loop(0, n // 2 - 2, pair, 0)
    for b in range(2):
        kcopy(n - 2 + b, (n - 2 + b) % NK).wait()
    for b in range(2):
        weights_of(score[b], weight[b])
    for b in range(2):
        scores_of(q_v, kbuf, score[b], n - 2 + b, (n - 2 + b) % NK)
    for b in range(2):
        vcopy(n - 4 + b, (n - 4 + b) % NV).wait()
    for b in range(2):
        seen_from(weight[b], vbuf, seen_v, n - 4 + b, (n - 4 + b) % NV)
    for b in range(2):
        weights_of(score[b], weight[b])
    for b in range(2):
        vcopy(n - 2 + b, (n - 2 + b) % NV).wait()
        seen_from(weight[b], vbuf, seen_v, n - 2 + b, (n - 2 + b) % NV)
    for step, *gs in TAIL:
        named[step](*gs)


def solution(mesh):
    n_dev = mesh.shape["tp"]

    def step(x, k_cache, v_cache, gain_a, wq, wo, gain_m, w_gate, w_up, w_down):
        n, d = x.shape
        cache = k_cache.shape[1]
        half = HEAD // 2
        angle = np.float32(cache - 1) * np.float32(THETA) ** (-np.arange(half, dtype=np.float32) / np.float32(half))
        angle = angle.astype(np.float32).astype(np.float64)
        cos, sin = np.cos(angle).astype(np.float32), np.sin(angle).astype(np.float32)
        turn = np.stack([np.concatenate([cos, cos]), np.concatenate([-sin, sin])])
        ff = w_gate.shape[1]
        rows = cache * 2
        out = pl.pallas_call(
            functools.partial(layer, n_dev),
            out_shape=jax.ShapeDtypeStruct((n // BLOCK, BLOCK, d), BF16),
            in_specs=[pl.BlockSpec(memory_space=pl.ANY)] * 11,
            out_specs=pl.BlockSpec(memory_space=pltpu.VMEM),
            scratch_shapes=[
                pltpu.VMEM((NK, rows, HEAD), BF16),
                pltpu.VMEM((NV, rows, HEAD), BF16),
                pltpu.VMEM((n // BLOCK, BLOCK, d), BF16),
                pltpu.VMEM((d // HEAD, HEAD), BF16),
                pltpu.VMEM((d // HEAD, HEAD), BF16),
                pltpu.VMEM((2, HEAD), F32),
                pltpu.VMEM((d, 2 * HEAD), BF16),
                pltpu.VMEM((2 * HEAD, d), BF16),
                pltpu.VMEM((d, ff), BF16),
                pltpu.VMEM((d, ff), BF16),
                pltpu.VMEM((ff, d), BF16),
                pltpu.VMEM((n, 2 * HEAD), F32),
                pltpu.VMEM((8, rows // 2), F32),
                pltpu.VMEM((8, rows // 2), F32),
                pltpu.VMEM((16, rows // 2), BF16),
                pltpu.VMEM((16, rows // 2), BF16),
                pltpu.VMEM((n, 8, HEAD), F32),
                *[pltpu.VMEM((g[1], d), BF16) for g in GROUPS],
                *[pltpu.VMEM((n_dev, g[1], d), BF16) for g in GROUPS],
                *[pltpu.VMEM((n_dev, g[1], d), BF16) for g in GROUPS],
                pltpu.SemaphoreType.DMA((NK,)),
                pltpu.SemaphoreType.DMA((NV,)),
                pltpu.SemaphoreType.DMA((9,)),
                pltpu.SemaphoreType.DMA((len(GROUPS), 2, n_dev)),
                pltpu.SemaphoreType.DMA((len(GROUPS), 2, n_dev)),
            ],
            compiler_params=pltpu.CompilerParams(vmem_limit_bytes=56 << 20, collective_id=0, has_side_effects=True),
        )(
            x.reshape(n // BLOCK, BLOCK, d),
            k_cache.reshape(n, rows, HEAD),
            v_cache.reshape(n, rows, HEAD),
            gain_a.reshape(-1, HEAD),
            wq,
            wo,
            gain_m.reshape(-1, HEAD),
            w_gate,
            w_up,
            w_down,
            jnp.asarray(turn),
        )
        return out.reshape(n, d)

    states, cache, columns, rows_of = P("dp", None), P("dp", None, "tp", None), P(None, "tp"), P("tp", None)
    return jax.shard_map(
        step,
        mesh=mesh,
        in_specs=(states, cache, cache, P(None), columns, rows_of, P(None), columns, columns, rows_of),
        out_specs=states,
        check_vma=False,
    )
```

```python
import functools

import jax
import jax.numpy as jnp
import numpy as np
from jax import lax
from jax.experimental import pallas as pl
from jax.experimental.pallas import tpu as pltpu
from jax.sharding import PartitionSpec as P

HEAD = 128
THETA = 10000
F32, BF16 = jnp.float32, jnp.bfloat16
LOG2E = 1.4426950408889634
BLOCK = 8
NK = NV = 8
GROUPS = [(0, 16), (16, 16), (32, 16), (48, 8), (56, 4), (60, 2), (62, 2)]
JOINED = [(0,), (1,), (2,), (3,), (4, 5, 6)]
STREAM = {
    7: [("attended", 0)],
    11: [("through", 0)],
    15: [("attended", 1), ("done", 0)],
    19: [("through", 1)],
    23: [("attended", 2), ("done", 1)],
    26: [("through", 2)],
    27: [("attended", 3)],
    29: [("attended", 4)],
}
LATE = [("attended", 5)]
TAIL = [("attended", 6), ("through", 3), ("done", 2), ("through", 4), ("done", 3), ("done", 4)]


def rows_in(m):
    return GROUPS[JOINED[m][0]][0], sum(GROUPS[g][1] for g in JOINED[m])


def normed(wide, gain):
    gain = gain.astype(F32)
    gain = jnp.concatenate([gain[c : c + 1] for c in range(gain.shape[0])], 1)
    scale = lax.rsqrt(jnp.mean(wide * wide, -1, keepdims=True) + 1e-6)
    return (wide * scale * gain).astype(BF16)


def twice(t):
    return jnp.concatenate([t, t], 0).astype(BF16)


def scores_of(q_ref, kbuf, s_ref, b, slot):
    row = q_ref[pl.ds(b, 1), :]
    q0 = jnp.broadcast_to(row[:, :HEAD], (16, HEAD))
    q1 = jnp.broadcast_to(row[:, HEAD:], (16, HEAD))
    r = lax.broadcasted_iota(jnp.int32, (16, HEAD), 0)
    q = jnp.where((r & 1) == 0, q0, q1)
    first = (r & 2) == 0
    lhs = jnp.concatenate([jnp.where(first, q, 0.0), jnp.where(first, 0.0, q)], 1).astype(BF16)
    for j in range(kbuf.shape[1] // 512):
        ka = kbuf[slot, 512 * j : 512 * j + 256, :]
        kb = kbuf[slot, 512 * j + 256 : 512 * j + 512, :]
        s = lax.dot_general(lhs, jnp.concatenate([ka, kb], 1), (((1,), (1,)), ((), ())), preferred_element_type=F32)
        s_ref[:, 256 * j : 256 * j + 256] = s[:8]


def weights_of(s_ref, p_ref):
    tiles = s_ref.shape[1] // 256
    r = lax.broadcasted_iota(jnp.int32, (8, 256), 0)
    c = lax.broadcasted_iota(jnp.int32, (8, 256), 1)
    mine = (r & 1) == (c & 1)
    t = [jnp.where(mine, s_ref[:, 256 * j : 256 * j + 256], -1e30) for j in range(tiles)]
    m = functools.reduce(jnp.maximum, t)
    m = jnp.max(jnp.maximum(m[:, :128], m[:, 128:]), 1, keepdims=True)
    m = jnp.broadcast_to(m, (8, 128))
    m = jnp.maximum(m, pltpu.roll(m, 2, 0))
    m = jnp.concatenate([m, m], 1)
    k = HEAD**-0.5 * LOG2E
    p = [jnp.exp2((x - m) * k) for x in t]
    l = functools.reduce(jnp.add, p)
    l = jnp.sum(l[:, :128] + l[:, 128:], 1, keepdims=True)
    l = jnp.broadcast_to(l, (8, 128))
    l = l + pltpu.roll(l, 2, 0)
    inv = 1.0 / l
    inv = jnp.concatenate([inv, inv], 1)
    for j in range(tiles):
        p_ref[:, 256 * j : 256 * j + 256] = twice(p[j] * inv)


def seen_from(p_ref, vbuf, seen_ref, b, slot):
    o = jnp.zeros((16, 256), F32)
    for j in range(vbuf.shape[1] // 512):
        va = vbuf[slot, 512 * j : 512 * j + 256, :]
        vb = vbuf[slot, 512 * j + 256 : 512 * j + 512, :]
        o = o + jnp.dot(p_ref[:, 256 * j : 256 * j + 256], jnp.concatenate([va, vb], 1), preferred_element_type=F32)
    o = o[:8]
    seen_ref[b] = o[:, :128] + pltpu.roll(o[:, 128:], 6, 0)


def layer(
    n_dev, x_ref, k_ref, v_ref, ga_ref, wq_ref, wo_ref, gm_ref, wg_ref, wu_ref, wd_ref, turn_ref, out_ref,
    kbuf, vbuf, x_v, ga_v, gm_v, turn_v, wq_v, wo_v, wg_v, wu_v, wd_v,
    q_v, s0_v, s1_v, p0_v, p1_v, seen_v, *rest,
):
    a, m = len(GROUPS), len(JOINED)
    h_v, hterm, yterm = rest[:m], rest[m : m + a], rest[m + a : 2 * m + a]
    ksem, vsem, wsem, send_sem, recv_sem = rest[2 * m + a :]
    me = lax.axis_index("tp")
    n = k_ref.shape[0]
    block = x_ref.shape[1]
    peers = [lax.rem(me + j, n_dev) for j in range(1, n_dev)]

    loads = [
        pltpu.make_async_copy(src, dst, wsem.at[i])
        for i, (src, dst) in enumerate(
            [
                (x_ref, x_v),
                (ga_ref, ga_v),
                (turn_ref, turn_v),
                (wq_ref, wq_v),
                (gm_ref, gm_v),
                (wo_ref, wo_v),
                (wg_ref, wg_v),
                (wu_ref, wu_v),
                (wd_ref, wd_v),
            ]
        )
    ]

    def kcopy(b, slot):
        return pltpu.make_async_copy(k_ref.at[b], kbuf.at[slot], ksem.at[slot])

    def vcopy(b, slot):
        return pltpu.make_async_copy(v_ref.at[b], vbuf.at[slot], vsem.at[slot])

    def rows_of(ref, first, count):
        if count >= block:
            return jnp.concatenate([ref[b] for b in range(first // block, (first + count) // block)], 0)
        return ref[first // block, first % block : first % block + count, :]

    def exchange(at, terms, peer, source):
        return pltpu.make_async_remote_copy(
            src_ref=terms.at[source],
            dst_ref=terms.at[source],
            send_sem=send_sem.at[at, peer],
            recv_sem=recv_sem.at[at, source],
            device_id={"tp": peer},
            device_id_type=pl.DeviceIdType.MESH,
        )

    def send(at, terms, out):
        terms[me] = out[: terms.shape[1]].astype(BF16)
        for peer in peers:
            exchange(at, terms, peer, me).start()

    def summed(at, terms):
        for source in peers:
            exchange(at, terms, me, source).wait_recv()
        for peer in peers:
            exchange(at, terms, peer, me).wait_send()
        return functools.reduce(jnp.add, [terms[i].astype(F32) for i in range(n_dev)])

    def filled(*parts):
        parts = list(parts)
        while sum(t.shape[0] for t in parts) < 16:
            parts.append(parts[-1])
        return jnp.concatenate(parts, 0).astype(BF16)

    def attended(g):
        if g == 0:
            loads[5].wait()
        first, count = GROUPS[g]
        seen = jnp.concatenate([seen_v[first : first + count, 0, :], seen_v[first : first + count, 1, :]], 1)
        send(g, hterm[g], jnp.dot(filled(seen), wo_v[...], preferred_element_type=F32))

    def through(m):
        if m == 0:
            for load in (loads[4], *loads[6:]):
                load.wait()
        parts, at = [], 0
        for g in JOINED[m]:
            first, count = GROUPS[g]
            h = (rows_of(x_v, first, count).astype(F32) + summed(g, hterm[g])).astype(BF16)
            h_v[m][at : at + count, :] = h
            at += count
            parts.append(normed(h.astype(F32), gm_v[...]).astype(F32))
        b = filled(jnp.concatenate(parts, 0))
        gate = jnp.dot(b, wg_v[...], preferred_element_type=F32)
        up = jnp.dot(b, wu_v[...], preferred_element_type=F32)
        out = jnp.dot((jax.nn.silu(gate) * up).astype(BF16), wd_v[...], preferred_element_type=F32)
        send(len(GROUPS) + m, yterm[m], out)

    def done(m):
        first, count = rows_in(m)
        y = (h_v[m][...].astype(F32) + summed(len(GROUPS) + m, yterm[m])).astype(BF16)
        for b in range(count // block):
            out_ref[first // block + b] = y[b * block : (b + 1) * block]

    def run(steps):
        for step, which in steps:
            {"attended": attended, "through": through, "done": done}[step](which)

    for load in loads[:4]:
        load.start()
    for s in range(NK):
        kcopy(s, s).start()
        vcopy(s, s).start()
    for load in loads[4:]:
        load.start()
    barrier = pltpu.get_barrier_semaphore()
    for peer in peers:
        pl.semaphore_signal(barrier, inc=1, device_id={"tp": peer}, device_id_type=pl.DeviceIdType.MESH)

    for load in loads[:4]:
        load.wait()
    wide = jnp.concatenate([x_v[b] for b in range(n // block)], 0).astype(F32)
    q = jnp.dot(normed(wide, ga_v[...]), wq_v[...], preferred_element_type=F32).astype(BF16).astype(F32)
    for i in range(2):
        t = q[:, HEAD * i : HEAD * (i + 1)]
        t = t * turn_v[0:1, :] + pltpu.roll(t, HEAD // 2, 1) * turn_v[1:2, :]
        q_v[:, HEAD * i : HEAD * (i + 1)] = t.astype(BF16).astype(F32)
    pl.semaphore_wait(barrier, n_dev - 1)

    score, weight = (s0_v, s1_v), (p0_v, p1_v)
    for b in range(2):
        kcopy(b, b).wait()
        scores_of(q_v, kbuf, score[b], b, b)
        kcopy(b + NK, b).start()

    def pair(p, carry):
        i = 2 * p
        for b in range(2):
            kcopy(i + b + 2, lax.rem(i + b + 2, NK)).wait()
            vcopy(i + b, lax.rem(i + b, NV)).wait()
        for b in range(2):
            weights_of(score[b], weight[b])
        for b in range(2):
            scores_of(q_v, kbuf, score[b], i + b + 2, lax.rem(i + b + 2, NK))
        for b in range(2):
            seen_from(weight[b], vbuf, seen_v, i + b, lax.rem(i + b, NV))

        @pl.when(i + 2 + NK < n)
        def _():
            for b in range(2):
                kcopy(i + b + 2 + NK, lax.rem(i + b + 2, NK)).start()

        @pl.when(i + NV < n)
        def _():
            for b in range(2):
                vcopy(i + b + NV, lax.rem(i + b, NV)).start()

        for at, steps in STREAM.items():

            @pl.when(p == at)
            def _():
                run(steps)

        return carry

    lax.fori_loop(0, n // 2 - 2, pair, 0)
    for b in range(2):
        kcopy(n - 2 + b, (n - 2 + b) % NK).wait()
    for b in range(2):
        weights_of(score[b], weight[b])
    for b in range(2):
        scores_of(q_v, kbuf, score[b], n - 2 + b, (n - 2 + b) % NK)
    for b in range(2):
        vcopy(n - 4 + b, (n - 4 + b) % NV).wait()
    for b in range(2):
        seen_from(weight[b], vbuf, seen_v, n - 4 + b, (n - 4 + b) % NV)
    for b in range(2):
        weights_of(score[b], weight[b])
    run(LATE)
    for b in range(2):
        vcopy(n - 2 + b, (n - 2 + b) % NV).wait()
        seen_from(weight[b], vbuf, seen_v, n - 2 + b, (n - 2 + b) % NV)
    run(TAIL)


def solution(mesh):
    n_dev = mesh.shape["tp"]

    def step(x, k_cache, v_cache, gain_a, wq, wo, gain_m, w_gate, w_up, w_down):
        n, d = x.shape
        cache = k_cache.shape[1]
        half = HEAD // 2
        angle = np.float32(cache - 1) * np.float32(THETA) ** (-np.arange(half, dtype=np.float32) / np.float32(half))
        angle = angle.astype(np.float32).astype(np.float64)
        cos, sin = np.cos(angle).astype(np.float32), np.sin(angle).astype(np.float32)
        turn = np.stack([np.concatenate([cos, cos]), np.concatenate([-sin, sin])])
        ff = w_gate.shape[1]
        rows = cache * 2
        out = pl.pallas_call(
            functools.partial(layer, n_dev),
            out_shape=jax.ShapeDtypeStruct((n // BLOCK, BLOCK, d), BF16),
            in_specs=[pl.BlockSpec(memory_space=pl.ANY)] * 11,
            out_specs=pl.BlockSpec(memory_space=pltpu.VMEM),
            scratch_shapes=[
                pltpu.VMEM((NK, rows, HEAD), BF16),
                pltpu.VMEM((NV, rows, HEAD), BF16),
                pltpu.VMEM((n // BLOCK, BLOCK, d), BF16),
                pltpu.VMEM((d // HEAD, HEAD), BF16),
                pltpu.VMEM((d // HEAD, HEAD), BF16),
                pltpu.VMEM((2, HEAD), F32),
                pltpu.VMEM((d, 2 * HEAD), BF16),
                pltpu.VMEM((2 * HEAD, d), BF16),
                pltpu.VMEM((d, ff), BF16),
                pltpu.VMEM((d, ff), BF16),
                pltpu.VMEM((ff, d), BF16),
                pltpu.VMEM((n, 2 * HEAD), F32),
                pltpu.VMEM((8, rows // 2), F32),
                pltpu.VMEM((8, rows // 2), F32),
                pltpu.VMEM((16, rows // 2), BF16),
                pltpu.VMEM((16, rows // 2), BF16),
                pltpu.VMEM((n, 8, HEAD), F32),
                *[pltpu.VMEM((rows_in(m)[1], d), BF16) for m in range(len(JOINED))],
                *[pltpu.VMEM((n_dev, g[1], d), BF16) for g in GROUPS],
                *[pltpu.VMEM((n_dev, rows_in(m)[1], d), BF16) for m in range(len(JOINED))],
                pltpu.SemaphoreType.DMA((NK,)),
                pltpu.SemaphoreType.DMA((NV,)),
                pltpu.SemaphoreType.DMA((9,)),
                pltpu.SemaphoreType.DMA((len(GROUPS) + len(JOINED), n_dev)),
                pltpu.SemaphoreType.DMA((len(GROUPS) + len(JOINED), n_dev)),
            ],
            compiler_params=pltpu.CompilerParams(vmem_limit_bytes=56 << 20, collective_id=0, has_side_effects=True),
        )(
            x.reshape(n // BLOCK, BLOCK, d),
            k_cache.reshape(n, rows, HEAD),
            v_cache.reshape(n, rows, HEAD),
            gain_a.reshape(-1, HEAD),
            wq,
            wo,
            gain_m.reshape(-1, HEAD),
            w_gate,
            w_up,
            w_down,
            jnp.asarray(turn),
        )
        return out.reshape(n, d)

    states, cache, columns, rows_of = P("dp", None), P("dp", None, "tp", None), P(None, "tp"), P("tp", None)
    return jax.shard_map(
        step,
        mesh=mesh,
        in_specs=(states, cache, cache, P(None), columns, rows_of, P(None), columns, columns, rows_of),
        out_specs=states,
        check_vma=False,
    )
```

```python
import functools

import jax
import jax.numpy as jnp
import numpy as np
from jax import lax
from jax.experimental import pallas as pl
from jax.experimental.pallas import tpu as pltpu
from jax.sharding import PartitionSpec as P

HEAD = 128
THETA = 10000
F32, BF16 = jnp.float32, jnp.bfloat16
LOG2E = 1.4426950408889634
BLOCK = 8
NK = NV = 8
GROUPS = [(0, 16), (16, 16), (32, 8), (40, 8), (48, 8), (56, 4), (60, 2), (62, 2)]
JOINED = [(0,), (1,), (2, 3), (4,), (5, 6, 7)]
PIECES = [1, 1, 1, 1, 2]
STREAM = {
    7: [("attended", 0)],
    11: [("through", 0)],
    15: [("attended", 1), ("done", 0)],
    19: [("through", 1), ("attended", 2)],
    23: [("attended", 3), ("done", 1)],
    25: [("through", 2)],
    27: [("attended", 4)],
}
LATE = [[("attended", 5)], [("attended", 6)]]
TAIL = [("attended", 7), ("through", 3), ("done", 2), ("through", 4), ("done", 3), ("done", 4)]


def rows_in(m):
    return GROUPS[JOINED[m][0]][0], sum(GROUPS[g][1] for g in JOINED[m])


def normed(wide, gain):
    gain = gain.astype(F32)
    gain = jnp.concatenate([gain[c : c + 1] for c in range(gain.shape[0])], 1)
    scale = lax.rsqrt(jnp.mean(wide * wide, -1, keepdims=True) + 1e-6)
    return (wide * scale * gain).astype(BF16)


def twice(t):
    return jnp.concatenate([t, t], 0).astype(BF16)


def scores_of(q_ref, kbuf, s_ref, b, slot):
    row = q_ref[pl.ds(b, 1), :]
    q0 = jnp.broadcast_to(row[:, :HEAD], (16, HEAD))
    q1 = jnp.broadcast_to(row[:, HEAD:], (16, HEAD))
    r = lax.broadcasted_iota(jnp.int32, (16, HEAD), 0)
    q = jnp.where((r & 1) == 0, q0, q1)
    first = (r & 2) == 0
    lhs = jnp.concatenate([jnp.where(first, q, 0.0), jnp.where(first, 0.0, q)], 1).astype(BF16)
    for j in range(kbuf.shape[1] // 512):
        ka = kbuf[slot, 512 * j : 512 * j + 256, :]
        kb = kbuf[slot, 512 * j + 256 : 512 * j + 512, :]
        s = lax.dot_general(lhs, jnp.concatenate([ka, kb], 1), (((1,), (1,)), ((), ())), preferred_element_type=F32)
        s_ref[:, 256 * j : 256 * j + 256] = s[:8]


def weights_of(s_ref, p_ref):
    tiles = s_ref.shape[1] // 256
    r = lax.broadcasted_iota(jnp.int32, (8, 256), 0)
    c = lax.broadcasted_iota(jnp.int32, (8, 256), 1)
    mine = (r & 1) == (c & 1)
    t = [jnp.where(mine, s_ref[:, 256 * j : 256 * j + 256], -1e30) for j in range(tiles)]
    m = functools.reduce(jnp.maximum, t)
    m = jnp.max(jnp.maximum(m[:, :128], m[:, 128:]), 1, keepdims=True)
    m = jnp.broadcast_to(m, (8, 128))
    m = jnp.maximum(m, pltpu.roll(m, 2, 0))
    m = jnp.concatenate([m, m], 1)
    k = HEAD**-0.5 * LOG2E
    p = [jnp.exp2((x - m) * k) for x in t]
    l = functools.reduce(jnp.add, p)
    l = jnp.sum(l[:, :128] + l[:, 128:], 1, keepdims=True)
    l = jnp.broadcast_to(l, (8, 128))
    l = l + pltpu.roll(l, 2, 0)
    inv = 1.0 / l
    inv = jnp.concatenate([inv, inv], 1)
    for j in range(tiles):
        p_ref[:, 256 * j : 256 * j + 256] = twice(p[j] * inv)


def seen_from(p_ref, vbuf, seen_ref, b, slot):
    o = jnp.zeros((16, 256), F32)
    for j in range(vbuf.shape[1] // 512):
        va = vbuf[slot, 512 * j : 512 * j + 256, :]
        vb = vbuf[slot, 512 * j + 256 : 512 * j + 512, :]
        o = o + jnp.dot(p_ref[:, 256 * j : 256 * j + 256], jnp.concatenate([va, vb], 1), preferred_element_type=F32)
    o = o[:8]
    seen_ref[b] = o[:, :128] + pltpu.roll(o[:, 128:], 6, 0)


def layer(
    n_dev, x_ref, k_ref, v_ref, ga_ref, wq_ref, wo_ref, gm_ref, wg_ref, wu_ref, wd_ref, turn_ref, out_ref,
    kbuf, vbuf, x_v, ga_v, gm_v, turn_v, wq_v, wo_v, wg_v, wu_v, wd_v,
    q_v, s0_v, s1_v, p0_v, p1_v, seen_v, *rest,
):
    a, m = len(GROUPS), len(JOINED)
    h_v, hterm, yterm = rest[:m], rest[m : m + a], rest[m + a : m + a + sum(PIECES)]
    ksem, vsem, wsem, send_sem, recv_sem = rest[m + a + sum(PIECES) :]
    me = lax.axis_index("tp")
    n = k_ref.shape[0]
    block = x_ref.shape[1]
    peers = [lax.rem(me + j, n_dev) for j in range(1, n_dev)]

    loads = [
        pltpu.make_async_copy(src, dst, wsem.at[i])
        for i, (src, dst) in enumerate(
            [
                (x_ref, x_v),
                (ga_ref, ga_v),
                (turn_ref, turn_v),
                (wq_ref, wq_v),
                (gm_ref, gm_v),
                (wo_ref, wo_v),
                (wg_ref, wg_v),
                (wu_ref, wu_v),
                (wd_ref, wd_v),
            ]
        )
    ]

    def kcopy(b, slot):
        return pltpu.make_async_copy(k_ref.at[b], kbuf.at[slot], ksem.at[slot])

    def vcopy(b, slot):
        return pltpu.make_async_copy(v_ref.at[b], vbuf.at[slot], vsem.at[slot])

    def rows_of(ref, first, count):
        if count >= block:
            return jnp.concatenate([ref[b] for b in range(first // block, (first + count) // block)], 0)
        return ref[first // block, first % block : first % block + count, :]

    def exchange(at, terms, peer, source):
        return pltpu.make_async_remote_copy(
            src_ref=terms.at[source],
            dst_ref=terms.at[source],
            send_sem=send_sem.at[at, peer],
            recv_sem=recv_sem.at[at, source],
            device_id={"tp": peer},
            device_id_type=pl.DeviceIdType.MESH,
        )

    def send(at, terms, out):
        terms[me] = out[: terms.shape[1]].astype(BF16)
        for peer in peers:
            exchange(at, terms, peer, me).start()

    def summed(at, terms):
        for source in peers:
            exchange(at, terms, me, source).wait_recv()
        for peer in peers:
            exchange(at, terms, peer, me).wait_send()
        return functools.reduce(jnp.add, [terms[i].astype(F32) for i in range(n_dev)])

    def filled(*parts):
        parts = list(parts)
        while sum(t.shape[0] for t in parts) < 16:
            parts.append(parts[-1])
        return jnp.concatenate(parts, 0).astype(BF16)

    def attended(g):
        if g == 0:
            loads[5].wait()
        first, count = GROUPS[g]
        seen = jnp.concatenate([seen_v[first : first + count, 0, :], seen_v[first : first + count, 1, :]], 1)
        send(g, hterm[g], jnp.dot(filled(seen), wo_v[...], preferred_element_type=F32))

    def pieces(m):
        width = x_ref.shape[2] // PIECES[m]
        return [(sum(PIECES[:m]) + i, pl.ds(i * width, width)) for i in range(PIECES[m])]

    def through(m):
        if m == 0:
            for load in (loads[4], *loads[6:]):
                load.wait()
        parts, at = [], 0
        for g in JOINED[m]:
            first, count = GROUPS[g]
            h = (rows_of(x_v, first, count).astype(F32) + summed(g, hterm[g])).astype(BF16)
            h_v[m][at : at + count, :] = h
            at += count
            parts.append(normed(h.astype(F32), gm_v[...]).astype(F32))
        b = filled(jnp.concatenate(parts, 0))
        gate = jnp.dot(b, wg_v[...], preferred_element_type=F32)
        up = jnp.dot(b, wu_v[...], preferred_element_type=F32)
        hidden = (jax.nn.silu(gate) * up).astype(BF16)
        for at, cols in pieces(m):
            send(len(GROUPS) + at, yterm[at], jnp.dot(hidden, wd_v[:, cols], preferred_element_type=F32))

    def done(m):
        first, count = rows_in(m)
        for at, cols in pieces(m):
            y = (h_v[m][:, cols].astype(F32) + summed(len(GROUPS) + at, yterm[at])).astype(BF16)
            for b in range(count // block):
                out_ref[first // block + b, :, cols] = y[b * block : (b + 1) * block]

    def run(steps):
        for step, which in steps:
            {"attended": attended, "through": through, "done": done}[step](which)

    for load in loads[:4]:
        load.start()
    for s in range(NK):
        kcopy(s, s).start()
        vcopy(s, s).start()
    for load in loads[4:]:
        load.start()
    barrier = pltpu.get_barrier_semaphore()
    for peer in peers:
        pl.semaphore_signal(barrier, inc=1, device_id={"tp": peer}, device_id_type=pl.DeviceIdType.MESH)

    for load in loads[:4]:
        load.wait()
    wide = jnp.concatenate([x_v[b] for b in range(n // block)], 0).astype(F32)
    q = jnp.dot(normed(wide, ga_v[...]), wq_v[...], preferred_element_type=F32).astype(BF16).astype(F32)
    for i in range(2):
        t = q[:, HEAD * i : HEAD * (i + 1)]
        t = t * turn_v[0:1, :] + pltpu.roll(t, HEAD // 2, 1) * turn_v[1:2, :]
        q_v[:, HEAD * i : HEAD * (i + 1)] = t.astype(BF16).astype(F32)
    pl.semaphore_wait(barrier, n_dev - 1)

    score, weight = (s0_v, s1_v), (p0_v, p1_v)
    for b in range(2):
        kcopy(b, b).wait()
        scores_of(q_v, kbuf, score[b], b, b)
        kcopy(b + NK, b).start()

    def pair(p, carry):
        i = 2 * p
        for b in range(2):
            kcopy(i + b + 2, lax.rem(i + b + 2, NK)).wait()
            vcopy(i + b, lax.rem(i + b, NV)).wait()
        for b in range(2):
            weights_of(score[b], weight[b])
        for b in range(2):
            scores_of(q_v, kbuf, score[b], i + b + 2, lax.rem(i + b + 2, NK))
        for b in range(2):
            seen_from(weight[b], vbuf, seen_v, i + b, lax.rem(i + b, NV))

        @pl.when(i + 2 + NK < n)
        def _():
            for b in range(2):
                kcopy(i + b + 2 + NK, lax.rem(i + b + 2, NK)).start()

        @pl.when(i + NV < n)
        def _():
            for b in range(2):
                vcopy(i + b + NV, lax.rem(i + b, NV)).start()

        for at, steps in STREAM.items():

            @pl.when(p == at)
            def _():
                run(steps)

        return carry

    lax.fori_loop(0, n // 2 - 3, pair, 0)
    for i, steps in zip((n - 6, n - 4), LATE):
        for b in range(i + 2, i + 4):
            kcopy(b, b % NK).wait()
        if i == n - 6:
            for b in range(2):
                weights_of(score[b], weight[b])
        for b in range(i + 2, i + 4):
            scores_of(q_v, kbuf, score[b % 2], b, b % NK)
        for b in range(i, i + 2):
            vcopy(b, b % NV).wait()
        for b in range(i, i + 2):
            seen_from(weight[b % 2], vbuf, seen_v, b, b % NV)
        for b in range(2):
            weights_of(score[b], weight[b])
        run(steps)
    for b in range(n - 2, n):
        vcopy(b, b % NV).wait()
        seen_from(weight[b % 2], vbuf, seen_v, b, b % NV)
    run(TAIL)


def solution(mesh):
    n_dev = mesh.shape["tp"]

    def step(x, k_cache, v_cache, gain_a, wq, wo, gain_m, w_gate, w_up, w_down):
        n, d = x.shape
        cache = k_cache.shape[1]
        half = HEAD // 2
        angle = np.float32(cache - 1) * np.float32(THETA) ** (-np.arange(half, dtype=np.float32) / np.float32(half))
        angle = angle.astype(np.float32).astype(np.float64)
        cos, sin = np.cos(angle).astype(np.float32), np.sin(angle).astype(np.float32)
        turn = np.stack([np.concatenate([cos, cos]), np.concatenate([-sin, sin])])
        ff = w_gate.shape[1]
        rows = cache * 2
        out = pl.pallas_call(
            functools.partial(layer, n_dev),
            out_shape=jax.ShapeDtypeStruct((n // BLOCK, BLOCK, d), BF16),
            in_specs=[pl.BlockSpec(memory_space=pl.ANY)] * 11,
            out_specs=pl.BlockSpec(memory_space=pltpu.VMEM),
            scratch_shapes=[
                pltpu.VMEM((NK, rows, HEAD), BF16),
                pltpu.VMEM((NV, rows, HEAD), BF16),
                pltpu.VMEM((n // BLOCK, BLOCK, d), BF16),
                pltpu.VMEM((d // HEAD, HEAD), BF16),
                pltpu.VMEM((d // HEAD, HEAD), BF16),
                pltpu.VMEM((2, HEAD), F32),
                pltpu.VMEM((d, 2 * HEAD), BF16),
                pltpu.VMEM((2 * HEAD, d), BF16),
                pltpu.VMEM((d, ff), BF16),
                pltpu.VMEM((d, ff), BF16),
                pltpu.VMEM((ff, d), BF16),
                pltpu.VMEM((n, 2 * HEAD), F32),
                pltpu.VMEM((8, rows // 2), F32),
                pltpu.VMEM((8, rows // 2), F32),
                pltpu.VMEM((16, rows // 2), BF16),
                pltpu.VMEM((16, rows // 2), BF16),
                pltpu.VMEM((n, 8, HEAD), F32),
                *[pltpu.VMEM((rows_in(m)[1], d), BF16) for m in range(len(JOINED))],
                *[pltpu.VMEM((n_dev, g[1], d), BF16) for g in GROUPS],
                *[pltpu.VMEM((n_dev, rows_in(m)[1], d // c), BF16) for m, c in enumerate(PIECES) for _ in range(c)],
                pltpu.SemaphoreType.DMA((NK,)),
                pltpu.SemaphoreType.DMA((NV,)),
                pltpu.SemaphoreType.DMA((9,)),
                pltpu.SemaphoreType.DMA((len(GROUPS) + sum(PIECES), n_dev)),
                pltpu.SemaphoreType.DMA((len(GROUPS) + sum(PIECES), n_dev)),
            ],
            compiler_params=pltpu.CompilerParams(vmem_limit_bytes=56 << 20, collective_id=0, has_side_effects=True),
        )(
            x.reshape(n // BLOCK, BLOCK, d),
            k_cache.reshape(n, rows, HEAD),
            v_cache.reshape(n, rows, HEAD),
            gain_a.reshape(-1, HEAD),
            wq,
            wo,
            gain_m.reshape(-1, HEAD),
            w_gate,
            w_up,
            w_down,
            jnp.asarray(turn),
        )
        return out.reshape(n, d)

    states, cache, columns, rows_of = P("dp", None), P("dp", None, "tp", None), P(None, "tp"), P("tp", None)
    return jax.shard_map(
        step,
        mesh=mesh,
        in_specs=(states, cache, cache, P(None), columns, rows_of, P(None), columns, columns, rows_of),
        out_specs=states,
        check_vma=False,
    )
```

```python
import functools

import jax
import jax.numpy as jnp
import numpy as np
from jax import lax
from jax.experimental import pallas as pl
from jax.experimental.pallas import tpu as pltpu
from jax.sharding import PartitionSpec as P

HEAD = 128
THETA = 10000
F32, BF16 = jnp.float32, jnp.bfloat16
LOG2E = 1.4426950408889634
BLOCK = 8
NK = NV = 8
GROUPS = [(0, 16), (16, 16), (32, 8), (40, 8), (48, 8), (56, 4), (60, 2), (62, 2)]
JOINED = [(0,), (1,), (2, 3), (4,), (5, 6, 7)]
PIECES = [1, 1, 1, 1, 2]
STREAM = {
    7: [("attended", 0)],
    11: [("through", 0)],
    15: [("attended", 1), ("done", 0)],
    19: [("through", 1), ("attended", 2)],
    23: [("attended", 3), ("done", 1)],
    25: [("through", 2)],
    27: [("attended", 4)],
}
LATE = [[("attended", 5)], [("attended", 6)]]
TAIL = [("attended", 7), ("through", 3), ("done", 2), ("through", 4), ("done", 3), ("done", 4)]


def rows_in(m):
    return GROUPS[JOINED[m][0]][0], sum(GROUPS[g][1] for g in JOINED[m])


def normed(wide, gain):
    gain = gain.astype(F32)
    gain = jnp.concatenate([gain[c : c + 1] for c in range(gain.shape[0])], 1)
    scale = lax.rsqrt(jnp.mean(wide * wide, -1, keepdims=True) + 1e-6)
    return (wide * scale * gain).astype(BF16)


def twice(t):
    return jnp.concatenate([t, t], 0).astype(BF16)


def scores_of(q_ref, kbuf, s_ref, b, slot):
    row = q_ref[pl.ds(b, 1), :]
    q0 = jnp.broadcast_to(row[:, :HEAD], (16, HEAD))
    q1 = jnp.broadcast_to(row[:, HEAD:], (16, HEAD))
    r = lax.broadcasted_iota(jnp.int32, (16, HEAD), 0)
    q = jnp.where((r & 1) == 0, q0, q1)
    first = (r & 2) == 0
    lhs = jnp.concatenate([jnp.where(first, q, 0.0), jnp.where(first, 0.0, q)], 1).astype(BF16)
    for j in range(kbuf.shape[1] // 512):
        ka = kbuf[slot, 512 * j : 512 * j + 256, :]
        kb = kbuf[slot, 512 * j + 256 : 512 * j + 512, :]
        s = lax.dot_general(lhs, jnp.concatenate([ka, kb], 1), (((1,), (1,)), ((), ())), preferred_element_type=F32)
        s_ref[:, 256 * j : 256 * j + 256] = s[:8]


def weights_of(s_ref, p_ref):
    tiles = s_ref.shape[1] // 256
    r = lax.broadcasted_iota(jnp.int32, (8, 256), 0)
    c = lax.broadcasted_iota(jnp.int32, (8, 256), 1)
    mine = (r & 1) == (c & 1)
    t = [jnp.where(mine, s_ref[:, 256 * j : 256 * j + 256], -1e30) for j in range(tiles)]
    m = functools.reduce(jnp.maximum, t)
    m = jnp.max(jnp.maximum(m[:, :128], m[:, 128:]), 1, keepdims=True)
    m = jnp.broadcast_to(m, (8, 128))
    m = jnp.maximum(m, pltpu.roll(m, 2, 0))
    m = jnp.concatenate([m, m], 1)
    k = HEAD**-0.5 * LOG2E
    p = [jnp.exp2((x - m) * k) for x in t]
    l = functools.reduce(jnp.add, p)
    l = jnp.sum(l[:, :128] + l[:, 128:], 1, keepdims=True)
    l = jnp.broadcast_to(l, (8, 128))
    l = l + pltpu.roll(l, 2, 0)
    inv = 1.0 / l
    inv = jnp.concatenate([inv, inv], 1)
    for j in range(tiles):
        p_ref[:, 256 * j : 256 * j + 256] = twice(p[j] * inv)


def seen_from(p_ref, vbuf, seen_ref, b, slot):
    o = jnp.zeros((16, 256), F32)
    for j in range(vbuf.shape[1] // 512):
        va = vbuf[slot, 512 * j : 512 * j + 256, :]
        vb = vbuf[slot, 512 * j + 256 : 512 * j + 512, :]
        o = o + jnp.dot(p_ref[:, 256 * j : 256 * j + 256], jnp.concatenate([va, vb], 1), preferred_element_type=F32)
    o = o[:8]
    seen_ref[b] = o[:, :128] + pltpu.roll(o[:, 128:], 6, 0)


def layer(
    n_dev, x_ref, k_ref, v_ref, ga_ref, wq_ref, wo_ref, gm_ref, wg_ref, wu_ref, wd_ref, turn_ref, out_ref,
    kbuf, vbuf, x_v, ga_v, gm_v, turn_v, wq_v, wo_v, wg_v, wu_v, wd_v,
    q_v, s0_v, s1_v, p0_v, p1_v, seen_v, *rest,
):
    a, m = len(GROUPS), len(JOINED)
    h_v, hterm, yterm = rest[:m], rest[m : m + a], rest[m + a : m + a + sum(PIECES)]
    ksem, vsem, wsem, send_sem, recv_sem = rest[m + a + sum(PIECES) :]
    me = lax.axis_index("tp")
    n = k_ref.shape[0]
    block = x_ref.shape[1]
    bits = [lax.rem(me // (1 << b), 2) for b in range(n_dev.bit_length() - 1)]
    far = sorted(range(1, n_dev), key=lambda j: (-bin(j >> 1).count("1"), j & 1, -j))
    peers = [sum(lax.rem(bit + (j >> b), 2) * (1 << b) for b, bit in enumerate(bits)) for j in far]

    loads = [
        pltpu.make_async_copy(src, dst, wsem.at[i])
        for i, (src, dst) in enumerate(
            [
                (x_ref, x_v),
                (ga_ref, ga_v),
                (turn_ref, turn_v),
                (wq_ref, wq_v),
                (gm_ref, gm_v),
                (wo_ref, wo_v),
                (wg_ref, wg_v),
                (wu_ref, wu_v),
                (wd_ref, wd_v),
            ]
        )
    ]

    def kcopy(b, slot):
        return pltpu.make_async_copy(k_ref.at[b], kbuf.at[slot], ksem.at[slot])

    def vcopy(b, slot):
        return pltpu.make_async_copy(v_ref.at[b], vbuf.at[slot], vsem.at[slot])

    def rows_of(ref, first, count):
        if count >= block:
            return jnp.concatenate([ref[b] for b in range(first // block, (first + count) // block)], 0)
        return ref[first // block, first % block : first % block + count, :]

    def exchange(at, terms, peer, source):
        return pltpu.make_async_remote_copy(
            src_ref=terms.at[source],
            dst_ref=terms.at[source],
            send_sem=send_sem.at[at, peer],
            recv_sem=recv_sem.at[at, source],
            device_id={"tp": peer},
            device_id_type=pl.DeviceIdType.MESH,
        )

    def send(at, terms, out):
        terms[me] = out[: terms.shape[1]].astype(BF16)
        for peer in peers:
            exchange(at, terms, peer, me).start()

    def summed(at, terms):
        for source in peers:
            exchange(at, terms, me, source).wait_recv()
        for peer in peers:
            exchange(at, terms, peer, me).wait_send()
        return functools.reduce(jnp.add, [terms[i].astype(F32) for i in range(n_dev)])

    def filled(*parts):
        parts = list(parts)
        while sum(t.shape[0] for t in parts) < 16:
            parts.append(parts[-1])
        return jnp.concatenate(parts, 0).astype(BF16)

    def attended(g):
        if g == 0:
            loads[5].wait()
        first, count = GROUPS[g]
        seen = jnp.concatenate([seen_v[first : first + count, 0, :], seen_v[first : first + count, 1, :]], 1)
        send(g, hterm[g], jnp.dot(filled(seen), wo_v[...], preferred_element_type=F32))

    def pieces(m):
        width = x_ref.shape[2] // PIECES[m]
        return [(sum(PIECES[:m]) + i, pl.ds(i * width, width)) for i in range(PIECES[m])]

    def through(m):
        if m == 0:
            for load in (loads[4], *loads[6:]):
                load.wait()
        parts, at = [], 0
        for g in JOINED[m]:
            first, count = GROUPS[g]
            h = (rows_of(x_v, first, count).astype(F32) + summed(g, hterm[g])).astype(BF16)
            h_v[m][at : at + count, :] = h
            at += count
            parts.append(normed(h.astype(F32), gm_v[...]).astype(F32))
        b = filled(jnp.concatenate(parts, 0))
        gate = jnp.dot(b, wg_v[...], preferred_element_type=F32)
        up = jnp.dot(b, wu_v[...], preferred_element_type=F32)
        hidden = (jax.nn.silu(gate) * up).astype(BF16)
        for at, cols in pieces(m):
            send(len(GROUPS) + at, yterm[at], jnp.dot(hidden, wd_v[:, cols], preferred_element_type=F32))

    def done(m):
        first, count = rows_in(m)
        for at, cols in pieces(m):
            y = (h_v[m][:, cols].astype(F32) + summed(len(GROUPS) + at, yterm[at])).astype(BF16)
            for b in range(count // block):
                out_ref[first // block + b, :, cols] = y[b * block : (b + 1) * block]

    def run(steps):
        for step, which in steps:
            {"attended": attended, "through": through, "done": done}[step](which)

    for load in loads[:4]:
        load.start()
    for s in range(NK):
        kcopy(s, s).start()
        vcopy(s, s).start()
    for load in loads[4:]:
        load.start()
    barrier = pltpu.get_barrier_semaphore()
    for peer in peers:
        pl.semaphore_signal(barrier, inc=1, device_id={"tp": peer}, device_id_type=pl.DeviceIdType.MESH)

    for load in loads[:4]:
        load.wait()
    wide = jnp.concatenate([x_v[b] for b in range(n // block)], 0).astype(F32)
    q = jnp.dot(normed(wide, ga_v[...]), wq_v[...], preferred_element_type=F32).astype(BF16).astype(F32)
    for i in range(2):
        t = q[:, HEAD * i : HEAD * (i + 1)]
        t = t * turn_v[0:1, :] + pltpu.roll(t, HEAD // 2, 1) * turn_v[1:2, :]
        q_v[:, HEAD * i : HEAD * (i + 1)] = t.astype(BF16).astype(F32)
    pl.semaphore_wait(barrier, n_dev - 1)

    score, weight = (s0_v, s1_v), (p0_v, p1_v)
    for b in range(2):
        kcopy(b, b).wait()
        scores_of(q_v, kbuf, score[b], b, b)
        kcopy(b + NK, b).start()

    def pair(p, carry):
        i = 2 * p
        for b in range(2):
            kcopy(i + b + 2, lax.rem(i + b + 2, NK)).wait()
            vcopy(i + b, lax.rem(i + b, NV)).wait()
        for b in range(2):
            weights_of(score[b], weight[b])
        for b in range(2):
            scores_of(q_v, kbuf, score[b], i + b + 2, lax.rem(i + b + 2, NK))
        for b in range(2):
            seen_from(weight[b], vbuf, seen_v, i + b, lax.rem(i + b, NV))

        @pl.when(i + 2 + NK < n)
        def _():
            for b in range(2):
                kcopy(i + b + 2 + NK, lax.rem(i + b + 2, NK)).start()

        @pl.when(i + NV < n)
        def _():
            for b in range(2):
                vcopy(i + b + NV, lax.rem(i + b, NV)).start()

        for at, steps in STREAM.items():

            @pl.when(p == at)
            def _():
                run(steps)

        return carry

    lax.fori_loop(0, n // 2 - 3, pair, 0)
    for i, steps in zip((n - 6, n - 4), LATE):
        for b in range(i + 2, i + 4):
            kcopy(b, b % NK).wait()
        if i == n - 6:
            for b in range(2):
                weights_of(score[b], weight[b])
        for b in range(i + 2, i + 4):
            scores_of(q_v, kbuf, score[b % 2], b, b % NK)
        for b in range(i, i + 2):
            vcopy(b, b % NV).wait()
        for b in range(i, i + 2):
            seen_from(weight[b % 2], vbuf, seen_v, b, b % NV)
        for b in range(2):
            weights_of(score[b], weight[b])
        run(steps)
    for b in range(n - 2, n):
        vcopy(b, b % NV).wait()
        seen_from(weight[b % 2], vbuf, seen_v, b, b % NV)
    run(TAIL)


def solution(mesh):
    n_dev = mesh.shape["tp"]

    def step(x, k_cache, v_cache, gain_a, wq, wo, gain_m, w_gate, w_up, w_down):
        n, d = x.shape
        cache = k_cache.shape[1]
        half = HEAD // 2
        angle = np.float32(cache - 1) * np.float32(THETA) ** (-np.arange(half, dtype=np.float32) / np.float32(half))
        angle = angle.astype(np.float32).astype(np.float64)
        cos, sin = np.cos(angle).astype(np.float32), np.sin(angle).astype(np.float32)
        turn = np.stack([np.concatenate([cos, cos]), np.concatenate([-sin, sin])])
        ff = w_gate.shape[1]
        rows = cache * 2
        out = pl.pallas_call(
            functools.partial(layer, n_dev),
            out_shape=jax.ShapeDtypeStruct((n // BLOCK, BLOCK, d), BF16),
            in_specs=[pl.BlockSpec(memory_space=pl.ANY)] * 11,
            out_specs=pl.BlockSpec(memory_space=pltpu.VMEM),
            scratch_shapes=[
                pltpu.VMEM((NK, rows, HEAD), BF16),
                pltpu.VMEM((NV, rows, HEAD), BF16),
                pltpu.VMEM((n // BLOCK, BLOCK, d), BF16),
                pltpu.VMEM((d // HEAD, HEAD), BF16),
                pltpu.VMEM((d // HEAD, HEAD), BF16),
                pltpu.VMEM((2, HEAD), F32),
                pltpu.VMEM((d, 2 * HEAD), BF16),
                pltpu.VMEM((2 * HEAD, d), BF16),
                pltpu.VMEM((d, ff), BF16),
                pltpu.VMEM((d, ff), BF16),
                pltpu.VMEM((ff, d), BF16),
                pltpu.VMEM((n, 2 * HEAD), F32),
                pltpu.VMEM((8, rows // 2), F32),
                pltpu.VMEM((8, rows // 2), F32),
                pltpu.VMEM((16, rows // 2), BF16),
                pltpu.VMEM((16, rows // 2), BF16),
                pltpu.VMEM((n, 8, HEAD), F32),
                *[pltpu.VMEM((rows_in(m)[1], d), BF16) for m in range(len(JOINED))],
                *[pltpu.VMEM((n_dev, g[1], d), BF16) for g in GROUPS],
                *[pltpu.VMEM((n_dev, rows_in(m)[1], d // c), BF16) for m, c in enumerate(PIECES) for _ in range(c)],
                pltpu.SemaphoreType.DMA((NK,)),
                pltpu.SemaphoreType.DMA((NV,)),
                pltpu.SemaphoreType.DMA((9,)),
                pltpu.SemaphoreType.DMA((len(GROUPS) + sum(PIECES), n_dev)),
                pltpu.SemaphoreType.DMA((len(GROUPS) + sum(PIECES), n_dev)),
            ],
            compiler_params=pltpu.CompilerParams(vmem_limit_bytes=56 << 20, collective_id=0, has_side_effects=True),
        )(
            x.reshape(n // BLOCK, BLOCK, d),
            k_cache.reshape(n, rows, HEAD),
            v_cache.reshape(n, rows, HEAD),
            gain_a.reshape(-1, HEAD),
            wq,
            wo,
            gain_m.reshape(-1, HEAD),
            w_gate,
            w_up,
            w_down,
            jnp.asarray(turn),
        )
        return out.reshape(n, d)

    states, cache, columns, rows_of = P("dp", None), P("dp", None, "tp", None), P(None, "tp"), P("tp", None)
    return jax.shard_map(
        step,
        mesh=mesh,
        in_specs=(states, cache, cache, P(None), columns, rows_of, P(None), columns, columns, rows_of),
        out_specs=states,
        check_vma=False,
    )
```
